32 devices in a mesh: row: 16 (over z, x, core), col: 2 (over y).
Axes of the slice: x: 2, y: 2, z: 4, core: 2. Of those that a mesh axis runs over, the one named last changes fastest.
Arguments:
- qkv: bfloat16 [256, 16, 3, 3072], P('row', 'col'), may hold values from -6 to 6
- cotangent: bfloat16 [256, 16, 3072], P('row', 'col'), may hold values from -6 to 6
- norm_gains: float32 [2, 128], replicated, may hold values from 0.1 to 1.9
- rel_table: float32 [24, 15, 15], replicated, may hold values from -6 to 250
- shifts: int32 [2], replicated, may hold values from 1 to 7
- mask_ids: int32 [256, 16], replicated, may hold values from 0 to 2
Outputs:
- attention: bfloat16 [256, 16, 3072], P('row', 'col')
- d_qkv: bfloat16 [256, 16, 3, 3072], P('row', 'col')
- d_gains: float32 [2, 128], replicated
- d_table: float32 [24, 15, 15], replicated
The draws below stay inside these ranges and needn't reach their ends.
All inputs are finite; a program needn't handle non-finite values.
Results may differ from the reference program's by a relative error of at most 0.0073.
Values may be sent and summed in bfloat16 or wider, within the bound.
A program may use at most 192 MiB of HBM per device.

```python
import math
import jax
import jax.numpy as jnp
from jax import lax

WIN = 8
NH = 24
HD = 128
FEATURES = 3072
SPAN = 15
ROWS = 256
COLS = 16


def draw_rel_table(key, part):
    base = jnp.clip(jax.random.normal(jax.random.fold_in(key, 11), (NH, SPAN, SPAN), jnp.float32), -6.0, 6.0)
    return base


def with_ends(array, own_key, low, top_value):
    spot = [jax.random.randint(jax.random.fold_in(own_key, axis), (), 0, length) for axis, length in enumerate(array.shape)]
    main_axis = array.shape.index(max(array.shape))
    next_to = spot[:main_axis] + [(spot[main_axis] + 1) % array.shape[main_axis]] + spot[main_axis + 1:]
    return array.at[tuple(spot)].set(low).at[tuple(next_to)].set(top_value)


def shard_levels(own_key, extent, shards, least, largest):
    def one(position, shards_of):
        steps = jax.random.uniform(jax.random.fold_in(jax.random.fold_in(own_key, 6), position), (shards_of,), jnp.float32, least / len(shards), largest / len(shards))
        return jnp.repeat(jnp.exp(steps), extent[position] // shards_of).reshape((-1,) + (1,) * (len(extent) - position - 1))

    gain = one(*shards[0])
    for cut in shards[1:]:
        gain = gain * one(*cut)
    return gain


def bell_draw(own_key, dims, scale, most, split=(), kind=jnp.bfloat16):
    array = scale * jax.random.normal(own_key, dims, jnp.float32)
    if split:
        array = array * shard_levels(own_key, dims, split, -0.22, 0.18)
    return jnp.clip(array, -most, most).astype(kind)


def setup_inputs(seed: int = 0) -> dict:
    seeds = jax.random.split(jax.random.key(seed), 7)
    qkv = bell_draw(seeds[0], (ROWS, COLS, 3, FEATURES), 1.0, 6.0, ((0, 16), (1, 2)))
    cotangent = bell_draw(seeds[1], (ROWS, COLS, FEATURES), 1.0, 6.0, ((0, 16), (1, 2)))
    norm_gains = jnp.clip(1.0 + 0.18 * jax.random.normal(seeds[2], (2, HD), jnp.float32), 0.1, 1.9)
    rel_table = draw_rel_table(jax.random.fold_in(seeds[6], 71), 0)
    shifts = jax.random.randint(seeds[4], (2,), 1, WIN).astype(jnp.int32)
    mask_ids = with_ends(jax.random.randint(seeds[5], (ROWS, COLS), 0, 3), jax.random.fold_in(seeds[5], 1), 0, 2).astype(jnp.int32)
    return {"qkv": qkv, "cotangent": cotangent, "norm_gains": norm_gains, "rel_table": rel_table, "shifts": shifts, "mask_ids": mask_ids}


EPSILON = 1e-06
NEG_FILL = -1e+30

def head_norm(inputs, gain_vec):
    values = inputs.astype(jnp.float32)
    average = lax.optimization_barrier(jnp.mean(values, axis=-1, keepdims=True))
    centred = values - average
    variance = lax.optimization_barrier(jnp.mean(centred * centred, axis=-1, keepdims=True))
    inv_sigma = lax.rsqrt(variance + EPSILON)
    x_hat = centred * inv_sigma
    return (x_hat, inv_sigma, (x_hat * gain_vec).astype(jnp.bfloat16))

def norm_back(x_hat, inv_sigma, d_normed, gain_vec):
    d_hat = d_normed * gain_vec
    first_mean = lax.optimization_barrier(jnp.mean(d_hat, axis=-1, keepdims=True))
    second_mean = lax.optimization_barrier(jnp.mean(d_hat * x_hat, axis=-1, keepdims=True))
    d_input = inv_sigma * (d_hat - first_mean - x_hat * second_mean)
    d_gain = lax.optimization_barrier(jnp.sum(d_normed * x_hat, axis=tuple(range(d_normed.ndim - 1))))
    return (d_input, d_gain)

def offset_table(window_size):
    span_count = 2 * window_size - 1
    places = jnp.arange(window_size * window_size, dtype=jnp.int32)
    row_pos = places // window_size
    col_pos = places % window_size
    code_grid = (row_pos[:, None] - row_pos[None, :] + window_size - 1) * span_count + (col_pos[:, None] - col_pos[None, :] + window_size - 1)
    codes = jnp.arange(span_count * span_count, dtype=jnp.int32)
    return (code_grid[:, :, None] == codes[None, None, :]).astype(jnp.float32)

def to_windows(field, window_size):
    row_count, col_count = (field.shape[0], field.shape[1])
    trailing = field.shape[2:]
    blocks = field.reshape((row_count // window_size, window_size, col_count // window_size, window_size) + trailing)
    blocks = jnp.moveaxis(blocks, 2, 1)
    return blocks.reshape((row_count // window_size * (col_count // window_size), window_size * window_size) + trailing)

def from_windows(blocks, window_size, row_count, col_count):
    trailing = blocks.shape[2:]
    field = blocks.reshape((row_count // window_size, col_count // window_size, window_size, window_size) + trailing)
    field = jnp.moveaxis(field, 1, 2)
    return field.reshape((row_count, col_count) + trailing)

def product(form, left, right):
    return jnp.einsum(form, left.astype(jnp.float32), right.astype(jnp.float32))

def window_core(q_norm, k_norm, values, grads, pos_bias, allowed, score_scale):
    scores = product('wqhd,wkhd->whqk', q_norm, k_norm) * score_scale + pos_bias[None]
    scores = jnp.where(allowed[:, None], scores, NEG_FILL)
    row_max = lax.optimization_barrier(jnp.max(scores, axis=-1, keepdims=True))
    weights = jnp.exp(scores - row_max)
    probs = weights / lax.optimization_barrier(jnp.sum(weights, axis=-1, keepdims=True))
    probs_b = probs.astype(jnp.bfloat16)
    output = product('whqk,wkhd->wqhd', probs_b, values)
    d_probs = product('wqhd,wkhd->whqk', grads, values)
    row_dot = lax.optimization_barrier(jnp.sum(probs * d_probs, axis=-1, keepdims=True))
    d_scores = probs * (d_probs - row_dot)
    d_scores_b = d_scores.astype(jnp.bfloat16)
    d_qnorm = product('whqk,wkhd->wqhd', d_scores_b, k_norm) * score_scale
    d_knorm = product('whqk,wqhd->wkhd', d_scores_b, q_norm) * score_scale
    d_value = product('whqk,wqhd->wkhd', probs_b, grads)
    return (output, d_qnorm, d_knorm, d_value, lax.optimization_barrier(jnp.sum(d_scores, axis=0)))

def reference(qkv, cotangent, norm_gains, rel_table, shifts, mask_ids):
    shift_row = shifts[0]
    shift_col = shifts[1]
    score_scale = 1.0 / math.sqrt(HD)
    one_hot = offset_table(WIN)
    pos_bias = jnp.einsum('hc,qkc->hqk', rel_table.reshape(NH, SPAN * SPAN), one_hot, precision=lax.Precision.HIGHEST)
    labels = jnp.roll(mask_ids, (-shift_row, -shift_col), (0, 1))

    def one_band(band_index):
        row_index = ((band_index * WIN + shift_row + jnp.arange(WIN, dtype=jnp.int32)) % ROWS).astype(jnp.int32)
        band_qkv = jnp.roll(jnp.take(qkv, row_index, axis=0), -shift_col, axis=1)
        band_grad = jnp.roll(jnp.take(cotangent, row_index, axis=0), -shift_col, axis=1)
        band_labels = lax.dynamic_slice_in_dim(labels, (band_index * WIN).astype(jnp.int32), WIN, 0)
        fields = band_qkv.reshape(WIN, COLS, 3, NH, HD)
        q_hat, q_inv, q_norm = head_norm(fields[:, :, 0], norm_gains[0])
        k_hat, k_inv, k_norm = head_norm(fields[:, :, 1], norm_gains[1])
        label_win = to_windows(band_labels, WIN)
        allowed = label_win[:, :, None] == label_win[:, None, :]
        output, d_qnorm, d_knorm, d_value, d_bias = window_core(to_windows(q_norm, WIN), to_windows(k_norm, WIN), to_windows(fields[:, :, 2], WIN), to_windows(band_grad.reshape(WIN, COLS, NH, HD), WIN), pos_bias, allowed, score_scale)
        output = from_windows(output, WIN, WIN, COLS)
        d_qnorm = from_windows(d_qnorm, WIN, WIN, COLS)
        d_knorm = from_windows(d_knorm, WIN, WIN, COLS)
        d_value = from_windows(d_value, WIN, WIN, COLS)
        d_query, dgain_q = norm_back(q_hat, q_inv, d_qnorm, norm_gains[0])
        d_key, dgain_k = norm_back(k_hat, k_inv, d_knorm, norm_gains[1])
        packed = jnp.stack([output, d_query, d_key, d_value], axis=2).reshape(WIN, COLS, 4, NH * HD).astype(jnp.bfloat16)
        return (packed, d_bias, jnp.stack([dgain_q, dgain_k]))
    packed, d_bias, d_gain = lax.map(one_band, jnp.arange(ROWS // WIN, dtype=jnp.int32))
    packed = jnp.roll(packed.reshape(ROWS, COLS, 4, NH * HD), (shift_row, shift_col), (0, 1))
    d_table = jnp.einsum('hqk,qkc->hc', lax.optimization_barrier(jnp.sum(d_bias, axis=0)), one_hot, precision=lax.Precision.HIGHEST)
    return (packed[:, :, 0], packed[:, :, 1:], lax.optimization_barrier(jnp.sum(d_gain, axis=0)), d_table.reshape(NH, SPAN, SPAN))
```

```python
import functools
import math

import jax
import jax.numpy as jnp
from jax import lax
from jax.experimental import pallas as pl
from jax.experimental.pallas import tpu as pltpu
from jax.sharding import PartitionSpec as P

EPSILON = 1e-06
NEG_FILL = -1e30
MESH = pl.DeviceIdType.MESH
F32 = jnp.float32
BF16 = jnp.bfloat16
LAG_COMPUTE = 3
LAG_ASSEMBLE = 2
LAG_FINAL = 1


def dot(a, b, lhs, rhs):
    return lax.dot_general(a, b, (((lhs,), (rhs,)), ((), ())), preferred_element_type=F32)


def window_kernel(
    steps,
    qkv,
    cot,
    gains,
    table,
    mask,
    att_out,
    dqkv_out,
    dgain,
    dskew,
    own_a,
    own_b,
    rowin_a,
    rowin_b,
    tokens,
    col_send,
    col_recv,
    results,
    out_send,
    out_recv,
    row_send,
    row_recv,
    out_a,
    out_b,
    neg,
    gather,
    scatter,
    load_sem,
    rowin_send_sem,
    rowin_recv_sem,
    col_sems,
    out_sems,
    row_sems,
    store_sem,
    *,
    row_dir,
    col_dir,
    width,
    win,
    heads,
    dim,
):
    chunks = own_a.shape[0]
    tile_rows, tile_cols = own_a.shape[1], own_a.shape[3]
    lanes = own_a.shape[4]
    half = win // 2
    size = tile_rows * tile_cols
    pad = width * tile_rows
    bands = tile_rows // win
    scale = 1.0 / math.sqrt(dim)
    rows = lax.axis_size("row")
    cols = lax.axis_size("col")
    me_row = lax.axis_index("row")
    me_col = lax.axis_index("col")
    row_step = steps[0]
    kept = size - pad

    def row_at(step):
        return (lax.rem(me_row + step + rows, rows), me_col)

    def col_at(step):
        return (me_row, lax.rem(me_col + step + cols, cols))

    def lane(g):
        return pl.ds(pl.multiple_of(g * lanes, lanes), lanes)

    first_row = 0 if row_dir > 0 else tile_rows - half
    halo_rows = pl.ds(first_row, half)

    def loads(g):
        return (
            pltpu.make_async_copy(qkv.at[:, :, :, lane(g)], own_a.at[g], load_sem.at[0, g]),
            pltpu.make_async_copy(cot.at[:, :, lane(g)], own_b.at[g], load_sem.at[1, g]),
        )

    def row_ins(g):
        return (
            pltpu.make_async_remote_copy(
                qkv.at[halo_rows, :, :, lane(g)],
                rowin_a.at[g],
                rowin_send_sem.at[0, g],
                rowin_recv_sem.at[0, g],
                device_id=row_at(-row_dir),
                device_id_type=MESH,
            ),
            pltpu.make_async_remote_copy(
                cot.at[halo_rows, :, lane(g)],
                rowin_b.at[g],
                rowin_send_sem.at[1, g],
                rowin_recv_sem.at[1, g],
                device_id=row_at(-row_dir),
                device_id_type=MESH,
            ),
        )

    def col_in(g):
        return pltpu.make_async_remote_copy(
            col_send.at[g],
            col_recv.at[g],
            col_sems.at[0, g],
            col_sems.at[1, g],
            device_id=col_at(-col_dir),
            device_id_type=MESH,
        )

    def col_back(g):
        return pltpu.make_async_remote_copy(
            out_send.at[g],
            out_recv.at[g],
            out_sems.at[0, g],
            out_sems.at[1, g],
            device_id=col_at(col_dir),
            device_id_type=MESH,
        )

    def row_back(g):
        return pltpu.make_async_remote_copy(
            row_send.at[g],
            row_recv.at[g],
            row_sems.at[0, g],
            row_sems.at[1, g],
            device_id=row_at(row_dir),
            device_id_type=MESH,
        )

    def stores(g):
        return (
            pltpu.make_async_copy(out_a.at[g], att_out.at[:, :, lane(g)], store_sem.at[0, g]),
            pltpu.make_async_copy(out_b.at[g], dqkv_out.at[:, :, :, lane(g)], store_sem.at[1, g]),
        )

    @pl.loop(0, chunks)
    def _(g):
        for copy in loads(g):
            copy.start()

    barrier = pltpu.get_barrier_semaphore()
    greeted = [row_at(1), row_at(-1), col_at(1)] + ([col_at(-1)] if cols > 2 else [])
    for neighbour in greeted:
        pl.semaphore_signal(barrier, inc=1, device_id=neighbour, device_id_type=MESH)
    pl.semaphore_wait(barrier, len(greeted))

    @pl.loop(0, chunks)
    def _(g):
        for copy in row_ins(g):
            copy.start()

    dgain[...] = jnp.zeros_like(dgain)

    iota = functools.partial(lax.broadcasted_iota, jnp.int32)

    def column_of(slot):
        if col_dir > 0:
            return jnp.where(slot < tile_cols - width, slot + width, slot - (tile_cols - width))
        return slot

    reach = size + half * tile_cols
    slot, source = iota((size, reach), 0), iota((size, reach), 1)
    row = slot % tile_rows + row_step
    column = column_of(slot // tile_rows)
    if row_dir > 0:
        wanted = row
    else:
        wanted = jnp.where(row < 0, row + half + tile_rows, row)
    gather[...] = (source == wanted * tile_cols + column).astype(BF16)
    spot, slot = iota((size, size), 0), iota((size, size), 1)
    row = (slot % tile_rows + row_step + tile_rows) % tile_rows
    scatter[...] = (spot == row * tile_cols + column_of(slot // tile_rows)).astype(BF16)

    row_count, col_count = mask.shape[1], mask.shape[0]
    from_row = lax.rem(row_count + me_row * tile_rows + row_step, row_count)
    from_col = lax.rem(col_count + me_col * tile_cols + steps[1], col_count)
    pick = (from_row + iota((row_count, size), 1) % tile_rows) % row_count
    pick = (iota((row_count, size), 0) == pick).astype(F32)
    by_row = dot(mask[...].astype(F32), pick, 1, 0)
    pick = (from_col + iota((col_count, size), 1) // tile_rows) % col_count
    across = jnp.where(iota((col_count, size), 0) == pick, by_row, 0.0)
    across = jnp.sum(across, axis=0, keepdims=True)
    band = (iota((1, size), 1) % tile_rows) // win
    code = jnp.broadcast_to(across * bands + band.astype(F32), (size, size))
    neg[...] = jnp.where(code == code.T, 0.0, NEG_FILL)

    gain_q, gain_k = gains[0:1, :], gains[1:2, :]
    head_lanes = [pl.ds(i * dim, dim) for i in range(heads)]

    def merge(g):
        for copy in loads(g):
            copy.wait()
        for copy in row_ins(g):
            copy.wait_recv()
        for f in range(4):
            own = own_a[g, :, f] if f < 3 else own_b[g]
            halo = rowin_a[g, :, f] if f < 3 else rowin_b[g]
            tiles = [own[r].astype(F32) for r in range(tile_rows)]
            tiles += [halo[r].astype(F32) for r in range(half)]
            placed = dot(gather[...], jnp.concatenate(tiles, axis=0).astype(BF16), 1, 0)
            placed = placed.astype(BF16)
            tokens[g, f] = placed[:kept]
            col_send[g, f] = placed[kept:]
        col_in(g).start()

    def normed(x, gain):
        centred = x - jnp.mean(x, axis=-1, keepdims=True)
        variance = jnp.mean(centred * centred, axis=-1, keepdims=True)
        inv = lax.rsqrt(variance + EPSILON)
        hat = centred * inv
        return hat, inv, (hat * gain).astype(BF16)

    def norm_back(hat, inv, dn, gain):
        g = dn * gain
        first = jnp.mean(g, axis=-1, keepdims=True)
        second = jnp.mean(g * hat, axis=-1, keepdims=True)
        return inv * (g - first - hat * second), jnp.sum(dn * hat, axis=0, keepdims=True)

    sub = 8
    lane_at = lax.broadcasted_iota(jnp.int32, (sub, size), 1)

    def attend(g, i):
        at = head_lanes[i]
        head = g * heads + i
        pairs = [(tokens[g, f, :, at], col_recv[g, f, :, at]) for f in range(4)]
        q, k, v, ct = [jnp.concatenate(pair[::col_dir], axis=0) for pair in pairs]
        q_hat, q_inv, qn = normed(q.astype(F32), gain_q)
        k_hat, k_inv, kn = normed(k.astype(F32), gain_k)
        base = jnp.broadcast_to(table[pl.ds(head, 1), :], (sub, 2 * size))
        base = pltpu.roll(base, 0, 1, stride=1, stride_axis=0)
        low, high = base[:, :size], base[:, size:]
        blocks = []
        for b in range(size // sub):
            if b == 0:
                blocks.append(low)
            else:
                blocks.append(
                    jnp.where(
                        lane_at < b * sub,
                        pltpu.roll(high, b * sub, 1),
                        pltpu.roll(low, b * sub, 1),
                    )
                )
        bias = jnp.concatenate(blocks, axis=0)
        s = dot(qn, kn, 1, 1) * scale + bias + neg[...]
        e = jnp.exp(s - jnp.max(s, axis=-1, keepdims=True))
        p = e * (1.0 / jnp.sum(e, axis=-1, keepdims=True))
        pb = p.astype(BF16)
        att = dot(pb, v, 1, 0)
        dp = dot(ct, v, 1, 1)
        ds = p * (dp - jnp.sum(p * dp, axis=-1, keepdims=True))
        dsb = ds.astype(BF16)
        dqn = dot(dsb, kn, 1, 0) * scale
        dkn = dot(dsb, qn, 0, 0) * scale
        dv = dot(pb, ct, 0, 0)
        low, high = ds[:sub], jnp.zeros((sub, size), F32)
        for b in range(1, size // sub):
            moved = pltpu.roll(ds[b * sub : (b + 1) * sub], size - b * sub, 1)
            inside = lane_at < size - b * sub
            low = low + jnp.where(inside, moved, 0.0)
            high = high + jnp.where(inside, 0.0, moved)
        dskew[head] = jnp.concatenate([low, high], axis=1)
        dq, gq = norm_back(q_hat, q_inv, dqn, gain_q)
        dk, gk = norm_back(k_hat, k_inv, dkn, gain_k)
        for f, value in enumerate((att, dq, dk, dv)):
            value = value.astype(BF16)
            if col_dir > 0:
                results[g, f, :, at] = value[:kept]
                out_send[g, f, :, at] = value[kept:]
            else:
                out_send[g, f, :, at] = value[:pad]
                results[g, f, :, at] = value[pad:]
        return jnp.concatenate([gq, gk], axis=0)

    def compute(g):
        col_in(g).wait_recv()
        parts = [attend(g, i) for i in range(heads)]
        dgain[...] += functools.reduce(jnp.add, parts)
        col_back(g).start()

    def assemble(g):
        col_back(g).wait_recv()
        for f in range(4):
            value = jnp.concatenate([results[g, f], out_recv[g, f]], axis=0)
            value = dot(scatter[...], value, 1, 0)
            for r in range(tile_rows):
                tile = value[r * tile_cols : (r + 1) * tile_cols].astype(BF16)
                if first_row <= r < first_row + half:
                    row_send[g, r - first_row, f] = tile
                elif f == 0:
                    out_a[g, r] = tile
                else:
                    out_b[g, r, f - 1] = tile
        row_back(g).start()

    def final(g):
        row_back(g).wait_recv()
        for f in range(4):
            for j in range(half):
                r = first_row + j
                foreign = (r < row_step) if row_dir > 0 else (r >= tile_rows + row_step)
                tile = jnp.where(
                    foreign, row_recv[g, j, f].astype(F32), row_send[g, j, f].astype(F32)
                ).astype(BF16)
                if f == 0:
                    out_a[g, r] = tile
                else:
                    out_b[g, r, f - 1] = tile
        for copy in stores(g):
            copy.start()

    lag_a = min(LAG_COMPUTE, chunks)
    lag_b = lag_a + LAG_ASSEMBLE
    lag_c = lag_b + LAG_FINAL

    @pl.loop(0, chunks + lag_c)
    def _(t):
        @pl.when(t < chunks)
        def _():
            merge(t)

        @pl.when(jnp.logical_and(t >= lag_c, t < chunks + lag_c))
        def _():
            final(t - lag_c)

        @pl.when(jnp.logical_and(t >= lag_b, t < chunks + lag_b))
        def _():
            assemble(t - lag_b)

        @pl.when(jnp.logical_and(t >= lag_a, t < chunks + lag_a))
        def _():
            compute(t - lag_a)

    @pl.loop(0, chunks)
    def _(g):
        for copy in row_ins(g):
            copy.wait_send()
        col_in(g).wait_send()
        col_back(g).wait_send()
        row_back(g).wait_send()
        for copy in stores(g):
            copy.wait()


def window_pass(
    qkv, cot, gains, table, mask, step, *, row_dir, col_dir, width, win, dim, call_id
):
    tile_rows, fields, tile_cols, features = qkv.shape
    head_count = features // dim
    heads = 2 if head_count % 2 == 0 else 1
    lanes = heads * dim
    chunks = head_count // heads
    half = win // 2
    size = tile_rows * tile_cols
    pad = width * tile_rows
    any_spec = pl.BlockSpec(memory_space=pl.ANY)
    vmem_spec = pl.BlockSpec(memory_space=pltpu.VMEM)
    vmem = pltpu.VMEM
    dma = pltpu.SemaphoreType.DMA
    return pl.pallas_call(
        functools.partial(
            window_kernel,
            row_dir=row_dir,
            col_dir=col_dir,
            width=width,
            win=win,
            heads=heads,
            dim=dim,
        ),
        in_specs=[pl.BlockSpec(memory_space=pltpu.SMEM), any_spec, any_spec]
        + [vmem_spec] * 3,
        out_specs=[any_spec, any_spec, vmem_spec, vmem_spec],
        out_shape=[
            jax.ShapeDtypeStruct(cot.shape, BF16),
            jax.ShapeDtypeStruct(qkv.shape, BF16),
            jax.ShapeDtypeStruct((2, dim), F32),
            jax.ShapeDtypeStruct((head_count, 8, 2 * size), F32),
        ],
        scratch_shapes=[
            vmem((chunks, tile_rows, fields, tile_cols, lanes), BF16),
            vmem((chunks, tile_rows, tile_cols, lanes), BF16),
            vmem((chunks, half, fields, tile_cols, lanes), BF16),
            vmem((chunks, half, tile_cols, lanes), BF16),
            vmem((chunks, 4, size - pad, lanes), BF16),
            vmem((chunks, 4, pad, lanes), BF16),
            vmem((chunks, 4, pad, lanes), BF16),
            vmem((chunks, 4, size - pad, lanes), BF16),
            vmem((chunks, 4, pad, lanes), BF16),
            vmem((chunks, 4, pad, lanes), BF16),
            vmem((chunks, half, 4, tile_cols, lanes), BF16),
            vmem((chunks, half, 4, tile_cols, lanes), BF16),
            vmem((chunks, tile_rows, tile_cols, lanes), BF16),
            vmem((chunks, tile_rows, fields, tile_cols, lanes), BF16),
            vmem((size, size), F32),
            vmem((size, size + half * tile_cols), BF16),
            vmem((size, size), BF16),
            dma((2, chunks)),
            dma((2, chunks)),
            dma((2, chunks)),
            dma((2, chunks)),
            dma((2, chunks)),
            dma((2, chunks)),
            dma((2, chunks)),
        ],
        compiler_params=pltpu.CompilerParams(
            collective_id=call_id, has_side_effects=True, vmem_limit_bytes=60 * 1024 * 1024
        ),
        name="windows",
    )(step, qkv, cot, gains, table, mask)


def total_over(value, axis):
    count = lax.axis_size(axis)
    if count & (count - 1):
        return lax.psum(value, axis)
    reach = 1
    while reach < count:
        value = value + lax.ppermute(value, axis, [(a, a ^ reach) for a in range(count)])
        reach *= 2
    return value


def local(qkv, cotangent, norm_gains, rel_table, shifts, mask_ids):
    head_count, span, _ = rel_table.shape
    dim = qkv.shape[3] // head_count
    win = (span + 1) // 2
    half = win // 2
    tile_rows = qkv.shape[0]
    size = tile_rows * qkv.shape[1]
    step = jnp.where(shifts <= half, shifts, shifts - win).astype(jnp.int32)
    gap = tile_rows - span
    reach = (win - 1) * (tile_rows + 1)
    flat = jnp.pad(
        rel_table[:, ::-1, ::-1].transpose(0, 2, 1), ((0, 0), (0, 0), (0, gap))
    ).reshape(head_count, span * tile_rows)
    flat = jnp.pad(flat, ((0, 0), (0, 2 * size - span * tile_rows)))
    table = jnp.roll(flat, -reach, axis=1)
    branches = []
    for row_dir in (1, -1):
        for col_step in (*range(1, half + 1), *range(1 - half, 0)):
            branches.append(
                functools.partial(
                    window_pass,
                    row_dir=row_dir,
                    col_dir=1 if col_step > 0 else -1,
                    width=abs(col_step),
                    win=win,
                    dim=dim,
                    call_id=len(branches),
                )
            )
    index = jnp.where(shifts[0] <= half, 0, win - 1) + shifts[1] - 1
    att, dqkv, dgain, dskew = lax.switch(
        index,
        branches,
        qkv.transpose(0, 2, 1, 3),
        cotangent,
        norm_gains,
        table,
        mask_ids.T,
        step,
    )
    dflat = sum(jnp.roll(dskew[:, j], -j, axis=1) for j in range(8))
    dflat = jnp.roll(dflat, reach, axis=1)[:, : span * tile_rows]
    sums = jnp.concatenate([dgain.reshape(-1), dflat.reshape(-1)])
    count = sums.shape[0]
    sums = jnp.pad(sums, (0, -count % 1024)).reshape(-1, 128)
    sums = total_over(total_over(sums, "col"), "row").reshape(-1)[:count]
    d_gains = sums[: 2 * dim].reshape(2, dim)
    d_table = sums[2 * dim :].reshape(head_count, span, tile_rows)[:, :, :span]
    d_table = d_table.transpose(0, 2, 1)[:, ::-1, ::-1]
    return (att, dqkv.transpose(0, 2, 1, 3), d_gains, d_table)


def solution(mesh):
    placed = (P("row", "col", None, None), P("row", "col", None), P(), P(), P(), P())
    return jax.shard_map(
        local,
        mesh=mesh,
        in_specs=placed,
        out_specs=(P("row", "col", None), P("row", "col", None, None), P(), P()),
        check_vma=False,
    )
```

```python
import functools
import math

import jax
import jax.numpy as jnp
from jax import lax
from jax.experimental import pallas as pl
from jax.experimental.pallas import tpu as pltpu
from jax.sharding import PartitionSpec as P

EPSILON = 1e-06
NEG_FILL = -1e30
MESH = pl.DeviceIdType.MESH
F32 = jnp.float32
BF16 = jnp.bfloat16
LAG_COMPUTE = 4
LAG_ASSEMBLE = 4
LAG_FINAL = 4


def dot(a, b, lhs, rhs):
    return lax.dot_general(a, b, (((lhs,), (rhs,)), ((), ())), preferred_element_type=F32)


def window_kernel(
    steps,
    qkv,
    cot,
    gains,
    table,
    mask,
    att_out,
    dqkv_out,
    dgain,
    dtable,
    own_a,
    own_b,
    rowin_a,
    rowin_b,
    tokens,
    col_send,
    col_recv,
    results,
    out_send,
    out_recv,
    row_send,
    row_recv,
    neg,
    gather,
    scatter,
    gain_sum,
    flat,
    across_table,
    skew,
    sum_send,
    sum_recv,
    load_sem,
    rowin_send_sem,
    rowin_recv_sem,
    col_sems,
    out_sems,
    row_sems,
    sum_sems,
    *,
    row_dir,
    col_dir,
    width,
    win,
    heads,
    dim,
):
    chunks = own_a.shape[0]
    tile_rows, tile_cols = own_a.shape[1], own_a.shape[3]
    lanes = own_a.shape[4]
    half = win // 2
    size = tile_rows * tile_cols
    pad = width * tile_rows
    bands = tile_rows // win
    scale = 1.0 / math.sqrt(dim)
    rows = lax.axis_size("row")
    cols = lax.axis_size("col")
    me_row = lax.axis_index("row")
    me_col = lax.axis_index("col")
    row_step = jnp.where(steps[0] <= half, steps[0], steps[0] - win)
    kept = size - pad

    def row_at(step):
        return (lax.rem(me_row + step + rows, rows), me_col)

    def col_at(step):
        return (me_row, lax.rem(me_col + step + cols, cols))

    def lane(g):
        return pl.ds(pl.multiple_of(g * lanes, lanes), lanes)

    first_row = 0 if row_dir > 0 else tile_rows - half
    halo_rows = pl.ds(first_row, half)

    def loads(g):
        return (
            pltpu.make_async_copy(qkv.at[:, :, :, lane(g)], own_a.at[g], load_sem.at[0, g]),
            pltpu.make_async_copy(cot.at[:, :, lane(g)], own_b.at[g], load_sem.at[1, g]),
        )

    def row_ins(g):
        return (
            pltpu.make_async_remote_copy(
                qkv.at[halo_rows, :, :, lane(g)],
                rowin_a.at[g],
                rowin_send_sem.at[0, g],
                rowin_recv_sem.at[0, g],
                device_id=row_at(-row_dir),
                device_id_type=MESH,
            ),
            pltpu.make_async_remote_copy(
                cot.at[halo_rows, :, lane(g)],
                rowin_b.at[g],
                rowin_send_sem.at[1, g],
                rowin_recv_sem.at[1, g],
                device_id=row_at(-row_dir),
                device_id_type=MESH,
            ),
        )

    def col_in(g):
        return pltpu.make_async_remote_copy(
            col_send.at[g],
            col_recv.at[g],
            col_sems.at[0, g],
            col_sems.at[1, g],
            device_id=col_at(-col_dir),
            device_id_type=MESH,
        )

    def col_back(g):
        return pltpu.make_async_remote_copy(
            out_send.at[g],
            out_recv.at[g],
            out_sems.at[0, g],
            out_sems.at[1, g],
            device_id=col_at(col_dir),
            device_id_type=MESH,
        )

    def row_back(g):
        return pltpu.make_async_remote_copy(
            row_send.at[g],
            row_recv.at[g],
            row_sems.at[0, g],
            row_sems.at[1, g],
            device_id=row_at(row_dir),
            device_id_type=MESH,
        )

    partners = []
    for axis, count, me in (("row", rows, me_row), ("col", cols, me_col)):
        reach = 1
        while reach < count:
            across = me + reach - 2 * reach * ((me // reach) % 2)
            partners.append((across, me_col) if axis == "row" else (me_row, across))
            reach *= 2

    def sum_copy(k):
        return pltpu.make_async_remote_copy(
            sum_send.at[k],
            sum_recv.at[k],
            sum_sems.at[0, k],
            sum_sems.at[1, k],
            device_id=partners[k],
            device_id_type=MESH,
        )

    @pl.loop(0, chunks)
    def _(g):
        for copy in loads(g):
            copy.start()

    barrier = pltpu.get_barrier_semaphore()
    row_rounds = rows.bit_length() - 1
    greeted = [row_at(1), row_at(-1), col_at(1)] + ([col_at(-1)] if cols > 2 else [])
    greeted += partners[1:row_rounds] + partners[row_rounds + 1 :]
    for neighbour in greeted:
        pl.semaphore_signal(barrier, inc=1, device_id=neighbour, device_id_type=MESH)
    pl.semaphore_wait(barrier, len(greeted))

    @pl.loop(0, chunks)
    def _(g):
        for copy in row_ins(g):
            copy.start()

    gain_sum[...] = jnp.zeros_like(gain_sum)
    span = table.shape[0]
    shift = (win - 1) * (tile_rows + 1)
    head_count = chunks * heads

    def spot_of(x, y):
        return (span - 1 - y) * tile_rows + span - 1 - x

    flat[...] = jnp.zeros_like(flat)

    @pl.loop(0, span)
    def _(x):
        for y in range(span):
            flat[pl.ds(spot_of(x, y), 1), 0:head_count] = table[x, y : y + 1, :]

    turned = jnp.concatenate([flat[:size].T, flat[size:].T], axis=1)
    across_table[...] = pltpu.roll(turned, 2 * size - shift, 1)

    iota = functools.partial(lax.broadcasted_iota, jnp.int32)

    def column_of(slot):
        if col_dir > 0:
            return jnp.where(slot < tile_cols - width, slot + width, slot - (tile_cols - width))
        return slot

    reach = size + half * tile_cols
    slot, source = iota((size, reach), 0), iota((size, reach), 1)
    row = slot % tile_rows + row_step
    column = column_of(slot // tile_rows)
    if row_dir > 0:
        wanted = row
    else:
        wanted = jnp.where(row < 0, row + half + tile_rows, row)
    gather[...] = (source == wanted * tile_cols + column).astype(BF16)
    spot, slot = iota((size, size), 0), iota((size, size), 1)
    row = (slot % tile_rows + row_step + tile_rows) % tile_rows
    scatter[...] = (spot == row * tile_cols + column_of(slot // tile_rows)).astype(BF16)

    row_count, col_count = mask.shape[1], mask.shape[0]
    from_row = lax.rem(row_count + me_row * tile_rows + row_step, row_count)
    from_col = lax.rem(col_count + me_col * tile_cols + jnp.where(steps[1] <= half, steps[1], steps[1] - win), col_count)
    pick = (from_row + iota((row_count, size), 1) % tile_rows) % row_count
    pick = (iota((row_count, size), 0) == pick).astype(F32)
    by_row = dot(mask[...].astype(F32), pick, 1, 0)
    pick = (from_col + iota((col_count, size), 1) // tile_rows) % col_count
    across = jnp.where(iota((col_count, size), 0) == pick, by_row, 0.0)
    across = jnp.sum(across, axis=0, keepdims=True)
    band = (iota((1, size), 1) % tile_rows) // win
    code = jnp.broadcast_to(across * bands + band.astype(F32), (size, size))
    neg[...] = jnp.where(code == code.T, 0.0, NEG_FILL)

    gain_q, gain_k = gains[0:1, :], gains[1:2, :]
    head_lanes = [pl.ds(i * dim, dim) for i in range(heads)]

    def merge(g):
        for copy in loads(g):
            copy.wait()
        for copy in row_ins(g):
            copy.wait_recv()
        for f in range(4):
            own = own_a[g, :, f] if f < 3 else own_b[g]
            halo = rowin_a[g, :, f] if f < 3 else rowin_b[g]
            tiles = [own[r].astype(F32) for r in range(tile_rows)]
            tiles += [halo[r].astype(F32) for r in range(half)]
            placed = dot(gather[...], jnp.concatenate(tiles, axis=0).astype(BF16), 1, 0)
            placed = placed.astype(BF16)
            tokens[g, f] = placed[:kept]
            col_send[g, f] = placed[kept:]
        col_in(g).start()

    def normed(x, gain):
        centred = x - jnp.mean(x, axis=-1, keepdims=True)
        variance = jnp.mean(centred * centred, axis=-1, keepdims=True)
        inv = lax.rsqrt(variance + EPSILON)
        hat = centred * inv
        return hat, inv, (hat * gain).astype(BF16)

    def norm_back(hat, inv, dn, gain):
        g = dn * gain
        first = jnp.mean(g, axis=-1, keepdims=True)
        second = jnp.mean(g * hat, axis=-1, keepdims=True)
        return inv * (g - first - hat * second), jnp.sum(dn * hat, axis=0, keepdims=True)

    sub = 8
    lane_at = lax.broadcasted_iota(jnp.int32, (sub, size), 1)

    def attend(g, i):
        at = head_lanes[i]
        head = g * heads + i
        pairs = [(tokens[g, f, :, at], col_recv[g, f, :, at]) for f in range(4)]
        q, k, v, ct = [jnp.concatenate(pair[::col_dir], axis=0) for pair in pairs]
        q_hat, q_inv, qn = normed(q.astype(F32), gain_q)
        k_hat, k_inv, kn = normed(k.astype(F32), gain_k)
        base = jnp.broadcast_to(across_table[pl.ds(head, 1), :], (sub, 2 * size))
        base = pltpu.roll(base, 0, 1, stride=1, stride_axis=0)
        low, high = base[:, :size], base[:, size:]
        blocks = []
        for b in range(size // sub):
            if b == 0:
                blocks.append(low)
            else:
                blocks.append(
                    jnp.where(
                        lane_at < b * sub,
                        pltpu.roll(high, b * sub, 1),
                        pltpu.roll(low, b * sub, 1),
                    )
                )
        bias = jnp.concatenate(blocks, axis=0)
        s = dot(qn, kn, 1, 1) * scale + bias + neg[...]
        e = jnp.exp(s - jnp.max(s, axis=-1, keepdims=True))
        p = e * (1.0 / jnp.sum(e, axis=-1, keepdims=True))
        pb = p.astype(BF16)
        att = dot(pb, v, 1, 0)
        dp = dot(ct, v, 1, 1)
        ds = p * (dp - jnp.sum(p * dp, axis=-1, keepdims=True))
        dsb = ds.astype(BF16)
        dqn = dot(dsb, kn, 1, 0) * scale
        dkn = dot(dsb, qn, 0, 0) * scale
        dv = dot(pb, ct, 0, 0)
        low, high = ds[:sub], jnp.zeros((sub, size), F32)
        for b in range(1, size // sub):
            moved = pltpu.roll(ds[b * sub : (b + 1) * sub], size - b * sub, 1)
            inside = lane_at < size - b * sub
            low = low + jnp.where(inside, moved, 0.0)
            high = high + jnp.where(inside, 0.0, moved)
        skew[0, pl.ds(head * sub, sub), :] = low
        skew[1, pl.ds(head * sub, sub), :] = high
        dq, gq = norm_back(q_hat, q_inv, dqn, gain_q)
        dk, gk = norm_back(k_hat, k_inv, dkn, gain_k)
        for f, value in enumerate((att, dq, dk, dv)):
            value = value.astype(BF16)
            if col_dir > 0:
                results[g, f, :, at] = value[:kept]
                out_send[g, f, :, at] = value[kept:]
            else:
                out_send[g, f, :, at] = value[:pad]
                results[g, f, :, at] = value[pad:]
        return jnp.concatenate([gq, gk], axis=0)

    def compute(g):
        col_in(g).wait_recv()
        parts = [attend(g, i) for i in range(heads)]
        gain_sum[...] += functools.reduce(jnp.add, parts)
        col_back(g).start()

    def assemble(g):
        col_back(g).wait_recv()
        for f in range(4):
            value = jnp.concatenate([results[g, f], out_recv[g, f]], axis=0)
            value = dot(scatter[...], value, 1, 0)
            for r in range(tile_rows):
                tile = value[r * tile_cols : (r + 1) * tile_cols].astype(BF16)
                if first_row <= r < first_row + half:
                    row_send[g, r - first_row, f] = tile
                elif f == 0:
                    att_out[r, :, lane(g)] = tile
                else:
                    dqkv_out[r, f - 1, :, lane(g)] = tile
        row_back(g).start()

    def final(g):
        row_back(g).wait_recv()
        for f in range(4):
            for j in range(half):
                r = first_row + j
                foreign = (r < row_step) if row_dir > 0 else (r >= tile_rows + row_step)
                tile = jnp.where(
                    foreign, row_recv[g, j, f].astype(F32), row_send[g, j, f].astype(F32)
                ).astype(BF16)
                if f == 0:
                    att_out[r, :, lane(g)] = tile
                else:
                    dqkv_out[r, f - 1, :, lane(g)] = tile

    def first_sum():
        total = jnp.zeros((head_count, 2 * size), F32)
        for j in range(sub):
            part = [skew[i, pl.ds(j, head_count, stride=sub), :] for i in range(2)]
            part = jnp.concatenate(part, axis=1)
            total = total + (pltpu.roll(part, 2 * size - j, 1) if j else part)
        total = pltpu.roll(total, shift, 1)
        gain = jnp.concatenate([gain_sum[0:1, :], gain_sum[1:2, :]], axis=1)
        rest = jnp.zeros((sum_send.shape[1] - head_count - 1, 2 * size), F32)
        sum_send[0] = jnp.concatenate([total, gain, rest], axis=0)
        sum_copy(0).start()

    def next_sum(k):
        sum_copy(k - 1).wait_recv()
        total = sum_send[k - 1] + sum_recv[k - 1]
        if k < len(partners):
            sum_send[k] = total
            sum_copy(k).start()
            return
        dgain[0:1, :] = total[head_count : head_count + 1, :dim]
        dgain[1:2, :] = total[head_count : head_count + 1, dim:]
        square = jnp.concatenate(
            [total, jnp.zeros((size - total.shape[0], 2 * size), F32)], axis=0
        )
        flat[0:size, :] = square[:, :size].T
        flat[size : 2 * size, :] = square[:, size:].T

        @pl.loop(0, span)
        def _(x):
            for y in range(span):
                dtable[x, y : y + 1, :] = flat[pl.ds(spot_of(x, y), 1), 0:head_count]

    lag_a = min(LAG_COMPUTE, chunks)
    lag_b = lag_a + LAG_ASSEMBLE
    lag_c = lag_b + LAG_FINAL

    rounds = len(partners)
    done = chunks + lag_a

    @pl.loop(0, max(chunks + lag_c, done + rounds + 1))
    def _(t):
        @pl.when(t < chunks)
        def _():
            merge(t)

        @pl.when(jnp.logical_and(t >= lag_c, t < chunks + lag_c))
        def _():
            final(t - lag_c)

        @pl.when(jnp.logical_and(t >= lag_b, t < chunks + lag_b))
        def _():
            assemble(t - lag_b)

        @pl.when(jnp.logical_and(t >= lag_a, t < chunks + lag_a))
        def _():
            compute(t - lag_a)

        for k in range(rounds + 1):

            @pl.when(t == done - 1 + k)
            def _(k=k):
                if k == 0:
                    first_sum()
                else:
                    next_sum(k)

    @pl.loop(0, chunks)
    def _(g):
        for copy in row_ins(g):
            copy.wait_send()
        col_in(g).wait_send()
        col_back(g).wait_send()
        row_back(g).wait_send()

    for k in range(rounds):
        sum_copy(k).wait_send()


def window_pass(
    steps, qkv, cot, gains, table, mask, *, row_dir, col_dir, width, win, dim, call_id
):
    tile_rows, fields, tile_cols, features = qkv.shape
    head_count = features // dim
    heads = 2 if head_count % 2 == 0 else 1
    lanes = heads * dim
    chunks = head_count // heads
    half = win // 2
    size = tile_rows * tile_cols
    pad = width * tile_rows
    rounds = sum(lax.axis_size(a).bit_length() - 1 for a in ("row", "col"))
    sum_rows = -(-(head_count + 1) // 8) * 8
    any_spec = pl.BlockSpec(memory_space=pl.ANY)
    vmem_spec = pl.BlockSpec(memory_space=pltpu.VMEM)
    vmem = pltpu.VMEM
    dma = pltpu.SemaphoreType.DMA
    return pl.pallas_call(
        functools.partial(
            window_kernel,
            row_dir=row_dir,
            col_dir=col_dir,
            width=width,
            win=win,
            heads=heads,
            dim=dim,
        ),
        in_specs=[pl.BlockSpec(memory_space=pltpu.SMEM), any_spec, any_spec]
        + [vmem_spec] * 3,
        out_specs=[vmem_spec] * 4,
        out_shape=[
            jax.ShapeDtypeStruct(cot.shape, BF16),
            jax.ShapeDtypeStruct(qkv.shape, BF16),
            jax.ShapeDtypeStruct((2, dim), F32),
            jax.ShapeDtypeStruct(table.shape, F32),
        ],
        scratch_shapes=[
            vmem((chunks, tile_rows, fields, tile_cols, lanes), BF16),
            vmem((chunks, tile_rows, tile_cols, lanes), BF16),
            vmem((chunks, half, fields, tile_cols, lanes), BF16),
            vmem((chunks, half, tile_cols, lanes), BF16),
            vmem((chunks, 4, size - pad, lanes), BF16),
            vmem((chunks, 4, pad, lanes), BF16),
            vmem((chunks, 4, pad, lanes), BF16),
            vmem((chunks, 4, size - pad, lanes), BF16),
            vmem((chunks, 4, pad, lanes), BF16),
            vmem((chunks, 4, pad, lanes), BF16),
            vmem((chunks, half, 4, tile_cols, lanes), BF16),
            vmem((chunks, half, 4, tile_cols, lanes), BF16),
            vmem((size, size), F32),
            vmem((size, size + half * tile_cols), BF16),
            vmem((size, size), BF16),
            vmem((2, dim), F32),
            vmem((2 * size, size), F32),
            vmem((size, 2 * size), F32),
            vmem((2, head_count * 8, size), F32),
            vmem((rounds, sum_rows, 2 * size), F32),
            vmem((rounds, sum_rows, 2 * size), F32),
            dma((2, chunks)),
            dma((2, chunks)),
            dma((2, chunks)),
            dma((2, chunks)),
            dma((2, chunks)),
            dma((2, chunks)),
            dma((2, rounds)),
        ],
        compiler_params=pltpu.CompilerParams(
            collective_id=call_id, has_side_effects=True, vmem_limit_bytes=60 * 1024 * 1024
        ),
        name="windows",
    )(steps, qkv, cot, gains, table, mask)


def local(qkv, cotangent, norm_gains, rel_table, shifts, mask_ids):
    head_count, span, _ = rel_table.shape
    dim = qkv.shape[3] // head_count
    win = (span + 1) // 2
    half = win // 2
    branches = []
    for row_dir in (1, -1):
        for col_step in (*range(1, half + 1), *range(1 - half, 0)):
            branches.append(
                functools.partial(
                    window_pass,
                    row_dir=row_dir,
                    col_dir=1 if col_step > 0 else -1,
                    width=abs(col_step),
                    win=win,
                    dim=dim,
                    call_id=len(branches),
                )
            )
    index = jnp.where(shifts[0] <= half, 0, win - 1) + shifts[1] - 1
    att, dqkv, dgain, dtable = lax.switch(
        index,
        branches,
        shifts,
        qkv.transpose(0, 2, 1, 3),
        cotangent,
        norm_gains,
        rel_table.transpose(1, 2, 0),
        mask_ids.T,
    )
    return (att, dqkv.transpose(0, 2, 1, 3), dgain, dtable.transpose(2, 0, 1))


def solution(mesh):
    placed = (P("row", "col", None, None), P("row", "col", None), P(), P(), P(), P())
    return jax.shard_map(
        local,
        mesh=mesh,
        in_specs=placed,
        out_specs=(P("row", "col", None), P("row", "col", None, None), P(), P()),
        check_vma=False,
    )
```

```python
import functools
import math

import jax
import jax.numpy as jnp
from jax import lax
from jax.experimental import pallas as pl
from jax.experimental.pallas import tpu as pltpu
from jax.sharding import PartitionSpec as P

EPSILON = 1e-06
NEG_FILL = -1e30
MESH = pl.DeviceIdType.MESH
F32 = jnp.float32
BF16 = jnp.bfloat16
HEADS = 2
LAG_COMPUTE = 3
LAG_RETURN = 3
LAG_FINAL = 4


def dot(a, b, lhs, rhs):
    return lax.dot_general(a, b, (((lhs,), (rhs,)), ((), ())), preferred_element_type=F32)


def window_kernel(
    steps,
    qkv,
    cot,
    gains,
    table,
    mask,
    att_out,
    dqkv_out,
    dgain,
    dtable,
    own_a,
    own_b,
    tokens,
    col_send,
    col_recv,
    row_send,
    row_recv,
    results,
    row_out,
    row_got,
    col_out,
    col_got,
    neg,
    split,
    strip,
    gather,
    strip_out,
    scatter_col,
    scatter,
    gain_sum,
    flat,
    across_table,
    skew,
    sum_send,
    sum_recv,
    load_sem,
    col_sems,
    row_sems,
    row_out_sems,
    col_out_sems,
    sum_sems,
    *,
    row_dir,
    col_dir,
    width,
    win,
    heads,
    dim,
):
    chunks = own_a.shape[0]
    tile_rows, tile_cols = own_a.shape[1], own_a.shape[3]
    lanes = own_a.shape[4]
    half = win // 2
    size = tile_rows * tile_cols
    pad = width * tile_rows
    bands = tile_rows // win
    scale = 1.0 / math.sqrt(dim)
    rows = lax.axis_size("row")
    cols = lax.axis_size("col")
    me_row = lax.axis_index("row")
    me_col = lax.axis_index("col")
    row_step = jnp.where(steps[0] <= half, steps[0], steps[0] - win)
    kept = size - pad

    def row_at(step):
        return (lax.rem(me_row + step + rows, rows), me_col)

    def col_at(step):
        return (me_row, lax.rem(me_col + step + cols, cols))

    def lane(g):
        return pl.ds(pl.multiple_of(g * lanes, lanes), lanes)

    first_row = 0 if row_dir > 0 else tile_rows - half

    def loads(g):
        return (
            pltpu.make_async_copy(qkv.at[:, :, :, lane(g)], own_a.at[g], load_sem.at[0, g]),
            pltpu.make_async_copy(cot.at[:, :, lane(g)], own_b.at[g], load_sem.at[1, g]),
        )

    def remote(source, target, sems, device):
        def copy(g):
            return pltpu.make_async_remote_copy(
                source.at[g],
                target.at[g],
                sems.at[0, g],
                sems.at[1, g],
                device_id=device,
                device_id_type=MESH,
            )

        return copy

    col_in = remote(col_send, col_recv, col_sems, col_at(-col_dir))
    row_in = remote(row_send, row_recv, row_sems, row_at(-row_dir))
    row_back = remote(row_out, row_got, row_out_sems, row_at(row_dir))
    col_back = remote(col_out, col_got, col_out_sems, col_at(col_dir))

    partners = []
    for axis, count, me in (("row", rows, me_row), ("col", cols, me_col)):
        reach = 1
        while reach < count:
            across = me + reach - 2 * reach * ((me // reach) % 2)
            partners.append((across, me_col) if axis == "row" else (me_row, across))
            reach *= 2

    def sum_copy(k):
        return pltpu.make_async_remote_copy(
            sum_send.at[k],
            sum_recv.at[k],
            sum_sems.at[0, k],
            sum_sems.at[1, k],
            device_id=partners[k],
            device_id_type=MESH,
        )

    @pl.loop(0, chunks)
    def _(g):
        for copy in loads(g):
            copy.start()

    barrier = pltpu.get_barrier_semaphore()
    row_rounds = rows.bit_length() - 1
    greeted = [row_at(1), row_at(-1), col_at(1)] + ([col_at(-1)] if cols > 2 else [])
    greeted += partners[1:row_rounds] + partners[row_rounds + 1 :]
    for neighbour in greeted:
        pl.semaphore_signal(barrier, inc=1, device_id=neighbour, device_id_type=MESH)
    pl.semaphore_wait(barrier, len(greeted))

    iota = functools.partial(lax.broadcasted_iota, jnp.int32)
    to, at = iota((size, size), 0), iota((size, size), 1)
    column = to // tile_rows
    if col_dir > 0:
        kept_columns = tile_cols - width
        column = jnp.where(column < kept_columns, column + width, column - kept_columns)
    split[...] = (at == (to % tile_rows) * tile_cols + column).astype(BF16)

    @pl.loop(0, chunks)
    def _(g):
        for copy in loads(g):
            copy.wait()
        for f in range(4):
            own = own_a[g, :, f] if f < 3 else own_b[g]
            tiles = [own[r].astype(F32) for r in range(tile_rows)]
            placed = dot(split[...], jnp.concatenate(tiles, axis=0).astype(BF16), 1, 0)
            placed = placed.astype(BF16)
            tokens[g, f] = placed[:kept]
            col_send[g, f] = placed[kept:]
        col_in(g).start()

    gain_sum[...] = jnp.zeros_like(gain_sum)
    span = table.shape[0]
    shift = (win - 1) * (tile_rows + 1)
    head_count = chunks * heads

    def spot_of(x, y):
        return (span - 1 - y) * tile_rows + span - 1 - x

    flat[...] = jnp.zeros_like(flat)

    @pl.loop(0, span)
    def _(x):
        for y in range(span):
            flat[pl.ds(spot_of(x, y), 1), 0:head_count] = table[x, y : y + 1, :]

    turned = jnp.concatenate([flat[:size].T, flat[size:].T], axis=1)
    across_table[...] = pltpu.roll(turned, 2 * size - shift, 1)

    slots = half * tile_cols

    def is_foreign(r):
        return (r < row_step) if row_dir > 0 else (r >= tile_rows + row_step)

    to, at = iota((slots, size), 0), iota((slots, size), 1)
    column, row = to // half, to % half + first_row
    strip[...] = (at == column * tile_rows + row).astype(BF16)
    row = (row - row_step + tile_rows) % tile_rows
    strip_out[...] = (at == column * tile_rows + row).astype(BF16)

    to, at = iota((size, size + slots), 0), iota((size, size + slots), 1)
    column, row = to // tile_rows, to % tile_rows + row_step
    halo = row - tile_rows if row_dir > 0 else row + half
    outside = (row >= tile_rows) if row_dir > 0 else (row < 0)
    wanted = jnp.where(outside, size + column * half + halo, column * tile_rows + row)
    gather[...] = (at == wanted).astype(BF16)

    skip = tile_cols - width if col_dir > 0 else 0
    to, at = iota((pad, pad + slots), 0), iota((pad, pad + slots), 1)
    column, row = to // tile_rows, to % tile_rows
    wanted = jnp.where(
        is_foreign(row),
        pad + (column + skip) * half + row - first_row,
        column * tile_rows + (row - row_step + tile_rows) % tile_rows,
    )
    scatter_col[...] = (at == wanted).astype(BF16)

    to, at = iota((size, size + slots), 0), iota((size, size + slots), 1)
    row, column = to // tile_cols, to % tile_cols
    if col_dir > 0:
        kept_column, held = column - width, column >= width
        back_column, place_column = column, column - width
    else:
        kept_column, held = column, column < tile_cols - width
        back_column, place_column = column - (tile_cols - width), column + width
    wanted = jnp.where(
        is_foreign(row),
        kept + place_column * half + row - first_row,
        kept_column * tile_rows + (row - row_step + tile_rows) % tile_rows,
    )
    wanted = jnp.where(held, wanted, kept + slots + back_column * tile_rows + row)
    scatter[...] = (at == wanted).astype(BF16)

    row_count, col_count = mask.shape[1], mask.shape[0]
    from_row = lax.rem(row_count + me_row * tile_rows + row_step, row_count)
    from_col = lax.rem(col_count + me_col * tile_cols + jnp.where(steps[1] <= half, steps[1], steps[1] - win), col_count)
    pick = (from_row + iota((row_count, size), 1) % tile_rows) % row_count
    pick = (iota((row_count, size), 0) == pick).astype(F32)
    by_row = dot(mask[...].astype(F32), pick, 1, 0)
    pick = (from_col + iota((col_count, size), 1) // tile_rows) % col_count
    across = jnp.where(iota((col_count, size), 0) == pick, by_row, 0.0)
    across = jnp.sum(across, axis=0, keepdims=True)
    band = (iota((1, size), 1) % tile_rows) // win
    code = jnp.broadcast_to(across * bands + band.astype(F32), (size, size))
    neg[...] = jnp.where(code == code.T, 0.0, NEG_FILL)

    gain_q, gain_k = gains[0:1, :], gains[1:2, :]
    head_lanes = [pl.ds(i * dim, dim) for i in range(heads)]

    def in_place(kept_part, other):
        pair = (kept_part, other)
        return jnp.concatenate(pair[::col_dir], axis=0)

    def merge(g):
        col_in(g).wait_recv()
        for f in range(4):
            both = in_place(tokens[g, f], col_recv[g, f])
            row_send[g, f] = dot(strip[...], both, 1, 0).astype(BF16)
        row_in(g).start()

    def normed(x, gain):
        centred = x - jnp.mean(x, axis=-1, keepdims=True)
        variance = jnp.mean(centred * centred, axis=-1, keepdims=True)
        inv = lax.rsqrt(variance + EPSILON)
        hat = centred * inv
        return hat, inv, (hat * gain).astype(BF16)

    def norm_back(hat, inv, dn, gain):
        g = dn * gain
        first = jnp.mean(g, axis=-1, keepdims=True)
        second = jnp.mean(g * hat, axis=-1, keepdims=True)
        return inv * (g - first - hat * second), jnp.sum(dn * hat, axis=0, keepdims=True)

    sub = 8
    lane_at = lax.broadcasted_iota(jnp.int32, (sub, size), 1)

    def attend(g, i, fields):
        at = head_lanes[i]
        head = g * heads + i
        q, k, v, ct = [field[:, i * dim : (i + 1) * dim] for field in fields]
        q_hat, q_inv, qn = normed(q.astype(F32), gain_q)
        k_hat, k_inv, kn = normed(k.astype(F32), gain_k)
        base = jnp.broadcast_to(across_table[pl.ds(head, 1), :], (sub, 2 * size))
        base = pltpu.roll(base, 0, 1, stride=1, stride_axis=0)
        low, high = base[:, :size], base[:, size:]
        blocks = []
        for b in range(size // sub):
            if b == 0:
                blocks.append(low)
            else:
                blocks.append(
                    jnp.where(
                        lane_at < b * sub,
                        pltpu.roll(high, b * sub, 1),
                        pltpu.roll(low, b * sub, 1),
                    )
                )
        bias = jnp.concatenate(blocks, axis=0)
        s = dot(qn, kn, 1, 1) * scale + bias + neg[...]
        e = jnp.exp(s - jnp.max(s, axis=-1, keepdims=True))
        p = e * (1.0 / jnp.sum(e, axis=-1, keepdims=True))
        pb = p.astype(BF16)
        att = dot(pb, v, 1, 0)
        dp = dot(ct, v, 1, 1)
        ds = p * (dp - jnp.sum(p * dp, axis=-1, keepdims=True))
        dsb = ds.astype(BF16)
        dqn = dot(dsb, kn, 1, 0) * scale
        dkn = dot(dsb, qn, 0, 0) * scale
        dv = dot(pb, ct, 0, 0)
        low, high = ds[:sub], jnp.zeros((sub, size), F32)
        for b in range(1, size // sub):
            moved = pltpu.roll(ds[b * sub : (b + 1) * sub], size - b * sub, 1)
            inside = lane_at < size - b * sub
            low = low + jnp.where(inside, moved, 0.0)
            high = high + jnp.where(inside, 0.0, moved)
        skew[0, pl.ds(head * sub, sub), :] = low
        skew[1, pl.ds(head * sub, sub), :] = high
        dq, gq = norm_back(q_hat, q_inv, dqn, gain_q)
        dk, gk = norm_back(k_hat, k_inv, dkn, gain_k)
        for f, value in enumerate((att, dq, dk, dv)):
            results[g, f, :, at] = value.astype(BF16)
        return jnp.concatenate([gq, gk], axis=0)

    def compute(g):
        row_in(g).wait_recv()
        fields = []
        for f in range(4):
            both = in_place(tokens[g, f], col_recv[g, f])
            both = jnp.concatenate([both, row_recv[g, f]], axis=0)
            fields.append(dot(gather[...], both, 1, 0).astype(BF16))
        parts = [attend(g, i, fields) for i in range(heads)]
        gain_sum[...] += functools.reduce(jnp.add, parts)
        for f in range(4):
            row_out[g, f] = dot(strip_out[...], results[g, f], 1, 0).astype(BF16)
        row_back(g).start()

    ours, theirs = pl.ds(0, kept), pl.ds(kept, pad)
    if col_dir < 0:
        ours, theirs = pl.ds(pad, kept), pl.ds(0, pad)

    def give_back(g):
        row_back(g).wait_recv()
        for f in range(4):
            both = jnp.concatenate([results[g, f, theirs], row_got[g, f]], axis=0)
            col_out[g, f] = dot(scatter_col[...], both, 1, 0).astype(BF16)
        col_back(g).start()

    def final(g):
        col_back(g).wait_recv()
        for f in range(4):
            parts = [results[g, f, ours], row_got[g, f], col_got[g, f]]
            value = dot(scatter[...], jnp.concatenate(parts, axis=0), 1, 0)
            for r in range(tile_rows):
                tile = value[r * tile_cols : (r + 1) * tile_cols].astype(BF16)
                if f == 0:
                    att_out[r, :, lane(g)] = tile
                else:
                    dqkv_out[r, f - 1, :, lane(g)] = tile

    def first_sum():
        total = jnp.zeros((head_count, 2 * size), F32)
        for j in range(sub):
            part = [skew[i, pl.ds(j, head_count, stride=sub), :] for i in range(2)]
            part = jnp.concatenate(part, axis=1)
            total = total + (pltpu.roll(part, 2 * size - j, 1) if j else part)
        total = pltpu.roll(total, shift, 1)
        gain = jnp.concatenate([gain_sum[0:1, :], gain_sum[1:2, :]], axis=1)
        rest = jnp.zeros((sum_send.shape[1] - head_count - 1, 2 * size), F32)
        sum_send[0] = jnp.concatenate([total, gain, rest], axis=0)
        sum_copy(0).start()

    def next_sum(k):
        sum_copy(k - 1).wait_recv()
        total = sum_send[k - 1] + sum_recv[k - 1]
        if k < len(partners):
            sum_send[k] = total
            sum_copy(k).start()
            return
        dgain[0:1, :] = total[head_count : head_count + 1, :dim]
        dgain[1:2, :] = total[head_count : head_count + 1, dim:]
        square = jnp.concatenate(
            [total, jnp.zeros((size - total.shape[0], 2 * size), F32)], axis=0
        )
        flat[0:size, :] = square[:, :size].T
        flat[size : 2 * size, :] = square[:, size:].T

        @pl.loop(0, span)
        def _(x):
            for y in range(span):
                dtable[x, y : y + 1, :] = flat[pl.ds(spot_of(x, y), 1), 0:head_count]

    lag_a = min(LAG_COMPUTE, chunks)
    lag_b = lag_a + LAG_RETURN
    lag_c = lag_b + LAG_FINAL

    rounds = len(partners)
    done = chunks + lag_a

    @pl.loop(0, max(chunks + lag_c, done + rounds + 1))
    def _(t):
        @pl.when(t < chunks)
        def _():
            merge(t)

        @pl.when(jnp.logical_and(t >= lag_b, t < chunks + lag_b))
        def _():
            give_back(t - lag_b)

        @pl.when(jnp.logical_and(t >= lag_a, t < chunks + lag_a))
        def _():
            compute(t - lag_a)

        @pl.when(jnp.logical_and(t >= lag_c, t < chunks + lag_c))
        def _():
            final(t - lag_c)

        for k in range(rounds + 1):

            @pl.when(t == done - 1 + k)
            def _(k=k):
                if k == 0:
                    first_sum()
                else:
                    next_sum(k)

    @pl.loop(0, chunks)
    def _(g):
        for copy in (col_in, row_in, row_back, col_back):
            copy(g).wait_send()

    for k in range(rounds):
        sum_copy(k).wait_send()


def window_pass(
    steps, qkv, cot, gains, table, mask, *, row_dir, col_dir, width, win, dim, call_id
):
    tile_rows, fields, tile_cols, features = qkv.shape
    head_count = features // dim
    heads = HEADS if head_count % HEADS == 0 else 1
    lanes = heads * dim
    chunks = head_count // heads
    half = win // 2
    slots = half * tile_cols
    size = tile_rows * tile_cols
    pad = width * tile_rows
    rounds = sum(lax.axis_size(a).bit_length() - 1 for a in ("row", "col"))
    sum_rows = -(-(head_count + 1) // 8) * 8
    any_spec = pl.BlockSpec(memory_space=pl.ANY)
    vmem_spec = pl.BlockSpec(memory_space=pltpu.VMEM)
    vmem = pltpu.VMEM
    dma = pltpu.SemaphoreType.DMA
    return pl.pallas_call(
        functools.partial(
            window_kernel,
            row_dir=row_dir,
            col_dir=col_dir,
            width=width,
            win=win,
            heads=heads,
            dim=dim,
        ),
        in_specs=[pl.BlockSpec(memory_space=pltpu.SMEM), any_spec, any_spec]
        + [vmem_spec] * 3,
        out_specs=[vmem_spec] * 4,
        out_shape=[
            jax.ShapeDtypeStruct(cot.shape, BF16),
            jax.ShapeDtypeStruct(qkv.shape, BF16),
            jax.ShapeDtypeStruct((2, dim), F32),
            jax.ShapeDtypeStruct(table.shape, F32),
        ],
        scratch_shapes=[
            vmem((chunks, tile_rows, fields, tile_cols, lanes), BF16),
            vmem((chunks, tile_rows, tile_cols, lanes), BF16),
            vmem((chunks, 4, size - pad, lanes), BF16),
            vmem((chunks, 4, pad, lanes), BF16),
            vmem((chunks, 4, pad, lanes), BF16),
            vmem((chunks, 4, slots, lanes), BF16),
            vmem((chunks, 4, slots, lanes), BF16),
            vmem((chunks, 4, size, lanes), BF16),
            vmem((chunks, 4, slots, lanes), BF16),
            vmem((chunks, 4, slots, lanes), BF16),
            vmem((chunks, 4, pad, lanes), BF16),
            vmem((chunks, 4, pad, lanes), BF16),
            vmem((size, size), F32),
            vmem((size, size), BF16),
            vmem((slots, size), BF16),
            vmem((size, size + slots), BF16),
            vmem((slots, size), BF16),
            vmem((pad, pad + slots), BF16),
            vmem((size, size + slots), BF16),
            vmem((2, dim), F32),
            vmem((2 * size, size), F32),
            vmem((size, 2 * size), F32),
            vmem((2, head_count * 8, size), F32),
            vmem((rounds, sum_rows, 2 * size), F32),
            vmem((rounds, sum_rows, 2 * size), F32),
            dma((2, chunks)),
            dma((2, chunks)),
            dma((2, chunks)),
            dma((2, chunks)),
            dma((2, chunks)),
            dma((2, rounds)),
        ],
        compiler_params=pltpu.CompilerParams(
            collective_id=call_id, has_side_effects=True, vmem_limit_bytes=60 * 1024 * 1024
        ),
        name="windows",
    )(steps, qkv, cot, gains, table, mask)


def local(qkv, cotangent, norm_gains, rel_table, shifts, mask_ids):
    head_count, span, _ = rel_table.shape
    dim = qkv.shape[3] // head_count
    win = (span + 1) // 2
    half = win // 2
    branches = []
    for row_dir in (1, -1):
        for col_step in (*range(1, half + 1), *range(1 - half, 0)):
            branches.append(
                functools.partial(
                    window_pass,
                    row_dir=row_dir,
                    col_dir=1 if col_step > 0 else -1,
                    width=abs(col_step),
                    win=win,
                    dim=dim,
                    call_id=len(branches),
                )
            )
    index = jnp.where(shifts[0] <= half, 0, win - 1) + shifts[1] - 1
    att, dqkv, dgain, dtable = lax.switch(
        index,
        branches,
        shifts,
        qkv.transpose(0, 2, 1, 3),
        cotangent,
        norm_gains,
        rel_table.transpose(1, 2, 0),
        mask_ids.T,
    )
    return (att, dqkv.transpose(0, 2, 1, 3), dgain, dtable.transpose(2, 0, 1))


def solution(mesh):
    placed = (P("row", "col", None, None), P("row", "col", None), P(), P(), P(), P())
    return jax.shard_map(
        local,
        mesh=mesh,
        in_specs=placed,
        out_specs=(P("row", "col", None), P("row", "col", None, None), P(), P()),
        check_vma=False,
    )
```

```python
import functools
import math

import jax
import jax.numpy as jnp
from jax import lax
from jax.experimental import pallas as pl
from jax.experimental.pallas import tpu as pltpu
from jax.sharding import PartitionSpec as P

EPSILON = 1e-06
NEG_FILL = -1e30
MESH = pl.DeviceIdType.MESH
F32 = jnp.float32
BF16 = jnp.bfloat16
HEADS = 2
LAG_COMPUTE = 4
LAG_RETURN = 4
LAG_FINAL = 4


def dot(a, b, lhs, rhs):
    return lax.dot_general(a, b, (((lhs,), (rhs,)), ((), ())), preferred_element_type=F32)


def window_kernel(
    steps,
    qkv,
    cot,
    gains,
    table,
    mask,
    att_out,
    dqkv_out,
    dgain,
    dtable,
    own_a,
    own_b,
    tokens,
    col_send,
    col_recv,
    row_send,
    row_recv,
    results,
    row_out,
    row_got,
    col_out,
    col_got,
    neg,
    split,
    strip,
    gather,
    strip_out,
    scatter_col,
    scatter,
    gain_sum,
    flat,
    across_table,
    skew,
    sum_send,
    sum_recv,
    load_sem,
    col_sems,
    row_sems,
    row_out_sems,
    col_out_sems,
    sum_sems,
    *,
    row_dir,
    col_dir,
    width,
    win,
    heads,
    dim,
):
    chunks = own_a.shape[0]
    tile_rows, tile_cols = own_a.shape[1], own_a.shape[3]
    lanes = own_a.shape[4]
    half = win // 2
    size = tile_rows * tile_cols
    pad = width * tile_rows
    bands = tile_rows // win
    scale = 1.0 / math.sqrt(dim)
    rows = lax.axis_size("row")
    cols = lax.axis_size("col")
    me_row = lax.axis_index("row")
    me_col = lax.axis_index("col")
    row_step = jnp.where(steps[0] <= half, steps[0], steps[0] - win)
    kept = size - pad

    def row_at(step):
        return (lax.rem(me_row + step + rows, rows), me_col)

    def col_at(step):
        return (me_row, lax.rem(me_col + step + cols, cols))

    def lane(g):
        return pl.ds(pl.multiple_of(g * lanes, lanes), lanes)

    first_row = 0 if row_dir > 0 else tile_rows - half

    def loads(g):
        return (
            pltpu.make_async_copy(qkv.at[:, :, :, lane(g)], own_a.at[g], load_sem.at[0, g]),
            pltpu.make_async_copy(cot.at[:, :, lane(g)], own_b.at[g], load_sem.at[1, g]),
        )

    def remote(source, target, sems, device):
        def copy(g):
            return pltpu.make_async_remote_copy(
                source.at[g],
                target.at[g],
                sems.at[0, g],
                sems.at[1, g],
                device_id=device,
                device_id_type=MESH,
            )

        return copy

    col_in = remote(col_send, col_recv, col_sems, col_at(-col_dir))
    row_in = remote(row_send, row_recv, row_sems, row_at(-row_dir))
    row_back = remote(row_out, row_got, row_out_sems, row_at(row_dir))
    col_back = remote(col_out, col_got, col_out_sems, col_at(col_dir))

    partners = []
    for axis, count, me in (("row", rows, me_row), ("col", cols, me_col)):
        reach = 1
        while reach < count:
            across = me + reach - 2 * reach * ((me // reach) % 2)
            partners.append((across, me_col) if axis == "row" else (me_row, across))
            reach *= 2

    def sum_copy(k):
        return pltpu.make_async_remote_copy(
            sum_send.at[k],
            sum_recv.at[k],
            sum_sems.at[0, k],
            sum_sems.at[1, k],
            device_id=partners[k],
            device_id_type=MESH,
        )

    @pl.loop(0, chunks)
    def _(g):
        for copy in loads(g):
            copy.start()

    barrier = pltpu.get_barrier_semaphore()
    row_rounds = rows.bit_length() - 1
    greeted = [row_at(1), row_at(-1), col_at(1)] + ([col_at(-1)] if cols > 2 else [])
    greeted += partners[1:row_rounds] + partners[row_rounds + 1 :]
    for neighbour in greeted:
        pl.semaphore_signal(barrier, inc=1, device_id=neighbour, device_id_type=MESH)
    pl.semaphore_wait(barrier, len(greeted))

    iota = functools.partial(lax.broadcasted_iota, jnp.int32)
    to, at = iota((size, size), 0), iota((size, size), 1)
    column = to // tile_rows
    if col_dir > 0:
        kept_columns = tile_cols - width
        column = jnp.where(column < kept_columns, column + width, column - kept_columns)
    split[...] = (at == (to % tile_rows) * tile_cols + column).astype(BF16)

    @pl.loop(0, chunks)
    def _(g):
        for copy in loads(g):
            copy.wait()
        for f in range(4):
            own = own_a[g, :, f] if f < 3 else own_b[g]
            tiles = [own[r].astype(F32) for r in range(tile_rows)]
            placed = dot(split[...], jnp.concatenate(tiles, axis=0).astype(BF16), 1, 0)
            placed = placed.astype(BF16)
            tokens[g, f] = placed[:kept]
            col_send[g, f] = placed[kept:]
        col_in(g).start()

    gain_sum[...] = jnp.zeros_like(gain_sum)
    span = table.shape[0]
    shift = (win - 1) * (tile_rows + 1)
    head_count = chunks * heads

    def spot_of(x, y):
        return (span - 1 - y) * tile_rows + span - 1 - x

    flat[...] = jnp.zeros_like(flat)

    @pl.loop(0, span)
    def _(x):
        for y in range(span):
            flat[pl.ds(spot_of(x, y), 1), 0:head_count] = table[x, y : y + 1, :]

    turned = jnp.concatenate([flat[:size].T, flat[size:].T], axis=1)
    across_table[...] = pltpu.roll(turned, 2 * size - shift, 1)

    slots = half * tile_cols

    def is_foreign(r):
        return (r < row_step) if row_dir > 0 else (r >= tile_rows + row_step)

    to, at = iota((slots, size), 0), iota((slots, size), 1)
    column, row = to // half, to % half + first_row
    strip[...] = (at == column * tile_rows + row).astype(BF16)
    row = (row - row_step + tile_rows) % tile_rows
    strip_out[...] = (at == column * tile_rows + row).astype(BF16)

    to, at = iota((size, size + slots), 0), iota((size, size + slots), 1)
    column, row = to // tile_rows, to % tile_rows + row_step
    halo = row - tile_rows if row_dir > 0 else row + half
    outside = (row >= tile_rows) if row_dir > 0 else (row < 0)
    wanted = jnp.where(outside, size + column * half + halo, column * tile_rows + row)
    gather[...] = (at == wanted).astype(BF16)

    skip = tile_cols - width if col_dir > 0 else 0
    to, at = iota((pad, pad + slots), 0), iota((pad, pad + slots), 1)
    column, row = to // tile_rows, to % tile_rows
    wanted = jnp.where(
        is_foreign(row),
        pad + (column + skip) * half + row - first_row,
        column * tile_rows + (row - row_step + tile_rows) % tile_rows,
    )
    scatter_col[...] = (at == wanted).astype(BF16)

    to, at = iota((size, size + slots), 0), iota((size, size + slots), 1)
    row, column = to // tile_cols, to % tile_cols
    if col_dir > 0:
        kept_column, held = column - width, column >= width
        back_column, place_column = column, column - width
    else:
        kept_column, held = column, column < tile_cols - width
        back_column, place_column = column - (tile_cols - width), column + width
    wanted = jnp.where(
        is_foreign(row),
        kept + place_column * half + row - first_row,
        kept_column * tile_rows + (row - row_step + tile_rows) % tile_rows,
    )
    wanted = jnp.where(held, wanted, kept + slots + back_column * tile_rows + row)
    scatter[...] = (at == wanted).astype(BF16)

    row_count, col_count = mask.shape[1], mask.shape[0]
    from_row = lax.rem(row_count + me_row * tile_rows + row_step, row_count)
    from_col = lax.rem(col_count + me_col * tile_cols + jnp.where(steps[1] <= half, steps[1], steps[1] - win), col_count)
    pick = (from_row + iota((row_count, size), 1) % tile_rows) % row_count
    pick = (iota((row_count, size), 0) == pick).astype(F32)
    by_row = dot(mask[...].astype(F32), pick, 1, 0)
    pick = (from_col + iota((col_count, size), 1) // tile_rows) % col_count
    across = jnp.where(iota((col_count, size), 0) == pick, by_row, 0.0)
    across = jnp.sum(across, axis=0, keepdims=True)
    band = (iota((1, size), 1) % tile_rows) // win
    code = jnp.broadcast_to(across * bands + band.astype(F32), (size, size))
    neg[...] = jnp.where(code == code.T, 0.0, NEG_FILL)

    gain_q, gain_k = gains[0:1, :], gains[1:2, :]
    head_lanes = [pl.ds(i * dim, dim) for i in range(heads)]

    def in_place(kept_part, other):
        pair = (kept_part, other)
        return jnp.concatenate(pair[::col_dir], axis=0)

    def merge(g):
        col_in(g).wait_recv()
        for f in range(4):
            both = in_place(tokens[g, f], col_recv[g, f])
            row_send[g, f] = dot(strip[...], both, 1, 0).astype(BF16)
        row_in(g).start()

    def normed(x, gain):
        centred = x - jnp.mean(x, axis=-1, keepdims=True)
        variance = jnp.mean(centred * centred, axis=-1, keepdims=True)
        inv = lax.rsqrt(variance + EPSILON)
        hat = centred * inv
        return hat, inv, (hat * gain).astype(BF16)

    def norm_back(hat, inv, dn, gain):
        g = dn * gain
        first = jnp.mean(g, axis=-1, keepdims=True)
        second = jnp.mean(g * hat, axis=-1, keepdims=True)
        return inv * (g - first - hat * second), jnp.sum(dn * hat, axis=0, keepdims=True)

    sub = 8
    lane_at = lax.broadcasted_iota(jnp.int32, (sub, size), 1)

    def bias_of(head):
        base = jnp.broadcast_to(across_table[pl.ds(head, 1), :], (sub, 2 * size))
        base = pltpu.roll(base, 0, 1, stride=1, stride_axis=0)
        low, high = base[:, :size], base[:, size:]
        blocks = [low]
        for b in range(1, size // sub):
            blocks.append(
                jnp.where(
                    lane_at < b * sub,
                    pltpu.roll(high, b * sub, 1),
                    pltpu.roll(low, b * sub, 1),
                )
            )
        return jnp.concatenate(blocks, axis=0)

    def fold(head, ds):
        low, high = ds[:sub], jnp.zeros((sub, size), F32)
        for b in range(1, size // sub):
            moved = pltpu.roll(ds[b * sub : (b + 1) * sub], size - b * sub, 1)
            inside = lane_at < size - b * sub
            low = low + jnp.where(inside, moved, 0.0)
            high = high + jnp.where(inside, 0.0, moved)
        skew[0, pl.ds(head * sub, sub), :] = low
        skew[1, pl.ds(head * sub, sub), :] = high

    def softmax(s):
        e = jnp.exp(s - jnp.max(s, axis=-1, keepdims=True))
        return e * (1.0 / jnp.sum(e, axis=-1, keepdims=True))

    def attend(g, fields):
        each = range(heads)
        split_heads = [[x[:, i * dim : (i + 1) * dim] for x in fields] for i in each]
        q, k, v, ct = zip(*split_heads)
        bias = [bias_of(g * heads + i) + neg[...] for i in each]
        qs = [normed(x.astype(F32), gain_q) for x in q]
        ks = [normed(x.astype(F32), gain_k) for x in k]
        qn, kn = [x[2] for x in qs], [x[2] for x in ks]
        s = [dot(qn[i], kn[i], 1, 1) for i in each]
        dp = [dot(ct[i], v[i], 1, 1) for i in each]
        p = [softmax(s[i] * scale + bias[i]) for i in each]
        ds = [p[i] * (dp[i] - jnp.sum(p[i] * dp[i], axis=-1, keepdims=True)) for i in each]
        pb = [x.astype(BF16) for x in p]
        dsb = [x.astype(BF16) for x in ds]
        dqn = [dot(dsb[i], kn[i], 1, 0) * scale for i in each]
        dkn = [dot(dsb[i], qn[i], 0, 0) * scale for i in each]
        att = [dot(pb[i], v[i], 1, 0) for i in each]
        dv = [dot(pb[i], ct[i], 0, 0) for i in each]
        total = 0.0
        for i, at in enumerate(head_lanes):
            fold(g * heads + i, ds[i])
            dq, gq = norm_back(qs[i][0], qs[i][1], dqn[i], gain_q)
            dk, gk = norm_back(ks[i][0], ks[i][1], dkn[i], gain_k)
            for f, value in enumerate((att[i], dq, dk, dv[i])):
                results[g, f, :, at] = value.astype(BF16)
            total = total + jnp.concatenate([gq, gk], axis=0)
        gain_sum[...] += total

    def compute(g):
        row_in(g).wait_recv()
        fields = []
        for f in range(4):
            both = in_place(tokens[g, f], col_recv[g, f])
            both = jnp.concatenate([both, row_recv[g, f]], axis=0)
            fields.append(dot(gather[...], both, 1, 0).astype(BF16))
        attend(g, fields)
        for f in range(4):
            row_out[g, f] = dot(strip_out[...], results[g, f], 1, 0).astype(BF16)
        row_back(g).start()

    ours, theirs = pl.ds(0, kept), pl.ds(kept, pad)
    if col_dir < 0:
        ours, theirs = pl.ds(pad, kept), pl.ds(0, pad)

    def give_back(g):
        row_back(g).wait_recv()
        for f in range(4):
            both = jnp.concatenate([results[g, f, theirs], row_got[g, f]], axis=0)
            col_out[g, f] = dot(scatter_col[...], both, 1, 0).astype(BF16)
        col_back(g).start()

    def final(g):
        col_back(g).wait_recv()
        for f in range(4):
            parts = [results[g, f, ours], row_got[g, f], col_got[g, f]]
            value = dot(scatter[...], jnp.concatenate(parts, axis=0), 1, 0)
            for r in range(tile_rows):
                tile = value[r * tile_cols : (r + 1) * tile_cols].astype(BF16)
                if f == 0:
                    att_out[r, :, lane(g)] = tile
                else:
                    dqkv_out[r, f - 1, :, lane(g)] = tile

    def first_sum():
        total = jnp.zeros((head_count, 2 * size), F32)
        for j in range(sub):
            part = [skew[i, pl.ds(j, head_count, stride=sub), :] for i in range(2)]
            part = jnp.concatenate(part, axis=1)
            total = total + (pltpu.roll(part, 2 * size - j, 1) if j else part)
        total = pltpu.roll(total, shift, 1)
        gain = jnp.concatenate([gain_sum[0:1, :], gain_sum[1:2, :]], axis=1)
        rest = jnp.zeros((sum_send.shape[1] - head_count - 1, 2 * size), F32)
        sum_send[0] = jnp.concatenate([total, gain, rest], axis=0)
        sum_copy(0).start()

    def next_sum(k):
        sum_copy(k - 1).wait_recv()
        total = sum_send[k - 1] + sum_recv[k - 1]
        if k < len(partners):
            sum_send[k] = total
            sum_copy(k).start()
            return
        dgain[0:1, :] = total[head_count : head_count + 1, :dim]
        dgain[1:2, :] = total[head_count : head_count + 1, dim:]
        square = jnp.concatenate(
            [total, jnp.zeros((size - total.shape[0], 2 * size), F32)], axis=0
        )
        flat[0:size, :] = square[:, :size].T
        flat[size : 2 * size, :] = square[:, size:].T

        @pl.loop(0, span)
        def _(x):
            for y in range(span):
                dtable[x, y : y + 1, :] = flat[pl.ds(spot_of(x, y), 1), 0:head_count]

    lag_a = min(LAG_COMPUTE, chunks)
    lag_b = lag_a + LAG_RETURN
    lag_c = lag_b + LAG_FINAL

    rounds = len(partners)
    done = chunks + lag_a

    @pl.loop(0, max(chunks + lag_c, done + rounds + 1))
    def _(t):
        @pl.when(t < chunks)
        def _():
            merge(t)

        @pl.when(jnp.logical_and(t >= lag_b, t < chunks + lag_b))
        def _():
            give_back(t - lag_b)

        @pl.when(jnp.logical_and(t >= lag_a, t < chunks + lag_a))
        def _():
            compute(t - lag_a)

        @pl.when(jnp.logical_and(t >= lag_c, t < chunks + lag_c))
        def _():
            final(t - lag_c)

        for k in range(rounds + 1):

            @pl.when(t == done - 1 + k)
            def _(k=k):
                if k == 0:
                    first_sum()
                else:
                    next_sum(k)

    @pl.loop(0, chunks)
    def _(g):
        for copy in (col_in, row_in, row_back, col_back):
            copy(g).wait_send()

    for k in range(rounds):
        sum_copy(k).wait_send()


def window_pass(
    steps, qkv, cot, gains, table, mask, *, row_dir, col_dir, width, win, dim, call_id
):
    tile_rows, fields, tile_cols, features = qkv.shape
    head_count = features // dim
    heads = HEADS if head_count % HEADS == 0 else 1
    lanes = heads * dim
    chunks = head_count // heads
    half = win // 2
    slots = half * tile_cols
    size = tile_rows * tile_cols
    pad = width * tile_rows
    rounds = sum(lax.axis_size(a).bit_length() - 1 for a in ("row", "col"))
    sum_rows = -(-(head_count + 1) // 8) * 8
    any_spec = pl.BlockSpec(memory_space=pl.ANY)
    vmem_spec = pl.BlockSpec(memory_space=pltpu.VMEM)
    vmem = pltpu.VMEM
    dma = pltpu.SemaphoreType.DMA
    return pl.pallas_call(
        functools.partial(
            window_kernel,
            row_dir=row_dir,
            col_dir=col_dir,
            width=width,
            win=win,
            heads=heads,
            dim=dim,
        ),
        in_specs=[pl.BlockSpec(memory_space=pltpu.SMEM), any_spec, any_spec]
        + [vmem_spec] * 3,
        out_specs=[vmem_spec] * 4,
        out_shape=[
            jax.ShapeDtypeStruct(cot.shape, BF16),
            jax.ShapeDtypeStruct(qkv.shape, BF16),
            jax.ShapeDtypeStruct((2, dim), F32),
            jax.ShapeDtypeStruct(table.shape, F32),
        ],
        scratch_shapes=[
            vmem((chunks, tile_rows, fields, tile_cols, lanes), BF16),
            vmem((chunks, tile_rows, tile_cols, lanes), BF16),
            vmem((chunks, 4, size - pad, lanes), BF16),
            vmem((chunks, 4, pad, lanes), BF16),
            vmem((chunks, 4, pad, lanes), BF16),
            vmem((chunks, 4, slots, lanes), BF16),
            vmem((chunks, 4, slots, lanes), BF16),
            vmem((chunks, 4, size, lanes), BF16),
            vmem((chunks, 4, slots, lanes), BF16),
            vmem((chunks, 4, slots, lanes), BF16),
            vmem((chunks, 4, pad, lanes), BF16),
            vmem((chunks, 4, pad, lanes), BF16),
            vmem((size, size), F32),
            vmem((size, size), BF16),
            vmem((slots, size), BF16),
            vmem((size, size + slots), BF16),
            vmem((slots, size), BF16),
            vmem((pad, pad + slots), BF16),
            vmem((size, size + slots), BF16),
            vmem((2, dim), F32),
            vmem((2 * size, size), F32),
            vmem((size, 2 * size), F32),
            vmem((2, head_count * 8, size), F32),
            vmem((rounds, sum_rows, 2 * size), F32),
            vmem((rounds, sum_rows, 2 * size), F32),
            dma((2, chunks)),
            dma((2, chunks)),
            dma((2, chunks)),
            dma((2, chunks)),
            dma((2, chunks)),
            dma((2, rounds)),
        ],
        compiler_params=pltpu.CompilerParams(
            collective_id=call_id, has_side_effects=True, vmem_limit_bytes=60 * 1024 * 1024
        ),
        name="windows",
    )(steps, qkv, cot, gains, table, mask)


def local(qkv, cotangent, norm_gains, rel_table, shifts, mask_ids):
    head_count, span, _ = rel_table.shape
    dim = qkv.shape[3] // head_count
    win = (span + 1) // 2
    half = win // 2
    branches = []
    for row_dir in (1, -1):
        for col_step in (*range(1, half + 1), *range(1 - half, 0)):
            branches.append(
                functools.partial(
                    window_pass,
                    row_dir=row_dir,
                    col_dir=1 if col_step > 0 else -1,
                    width=abs(col_step),
                    win=win,
                    dim=dim,
                    call_id=len(branches),
                )
            )
    index = jnp.where(shifts[0] <= half, 0, win - 1) + shifts[1] - 1
    att, dqkv, dgain, dtable = lax.switch(
        index,
        branches,
        shifts,
        qkv.transpose(0, 2, 1, 3),
        cotangent,
        norm_gains,
        rel_table.transpose(1, 2, 0),
        mask_ids.T,
    )
    return (att, dqkv.transpose(0, 2, 1, 3), dgain, dtable.transpose(2, 0, 1))


def solution(mesh):
    placed = (P("row", "col", None, None), P("row", "col", None), P(), P(), P(), P())
    return jax.shard_map(
        local,
        mesh=mesh,
        in_specs=placed,
        out_specs=(P("row", "col", None), P("row", "col", None, None), P(), P()),
        check_vma=False,
    )
```

```python
import functools
import math

import jax
import jax.numpy as jnp
from jax import lax
from jax.experimental import pallas as pl
from jax.experimental.pallas import tpu as pltpu
from jax.sharding import PartitionSpec as P

EPSILON = 1e-06
NEG_FILL = -1e30
MESH = pl.DeviceIdType.MESH
F32 = jnp.float32
BF16 = jnp.bfloat16
HEADS = 3
LAG_COMPUTE = 3
LAG_RETURN = 2
LAG_FINAL = 3


def dot(a, b, lhs, rhs):
    return lax.dot_general(a, b, (((lhs,), (rhs,)), ((), ())), preferred_element_type=F32)


def window_kernel(
    steps,
    qkv,
    cot,
    gains,
    table,
    mask,
    att_out,
    dqkv_out,
    dgain,
    dtable,
    own_a,
    own_b,
    tokens,
    col_send,
    col_recv,
    row_send,
    row_recv,
    results,
    row_out,
    row_got,
    col_out,
    col_got,
    neg,
    split,
    strip,
    gather,
    strip_out,
    scatter_col,
    scatter,
    gain_sum,
    flat,
    across_table,
    skew,
    sum_send,
    sum_recv,
    load_sem,
    col_sems,
    row_sems,
    row_out_sems,
    col_out_sems,
    sum_sems,
    *,
    row_dir,
    col_dir,
    width,
    win,
    heads,
    dim,
):
    chunks = own_a.shape[0]
    tile_rows, tile_cols = own_a.shape[1], own_a.shape[3]
    lanes = own_a.shape[4]
    half = win // 2
    size = tile_rows * tile_cols
    pad = width * tile_rows
    bands = tile_rows // win
    scale = 1.0 / math.sqrt(dim)
    rows = lax.axis_size("row")
    cols = lax.axis_size("col")
    me_row = lax.axis_index("row")
    me_col = lax.axis_index("col")
    row_step = jnp.where(steps[0] <= half, steps[0], steps[0] - win)
    kept = size - pad

    def row_at(step):
        return (lax.rem(me_row + step + rows, rows), me_col)

    def col_at(step):
        return (me_row, lax.rem(me_col + step + cols, cols))

    def lane(g):
        return pl.ds(pl.multiple_of(g * lanes, lanes), lanes)

    first_row = 0 if row_dir > 0 else tile_rows - half

    def loads(g):
        return (
            pltpu.make_async_copy(qkv.at[:, :, :, lane(g)], own_a.at[g], load_sem.at[0, g]),
            pltpu.make_async_copy(cot.at[:, :, lane(g)], own_b.at[g], load_sem.at[1, g]),
        )

    def remote(source, target, sems, device):
        def copy(g):
            return pltpu.make_async_remote_copy(
                source.at[g],
                target.at[g],
                sems.at[0, g],
                sems.at[1, g],
                device_id=device,
                device_id_type=MESH,
            )

        return copy

    col_in = remote(col_send, col_recv, col_sems, col_at(-col_dir))
    row_in = remote(row_send, row_recv, row_sems, row_at(-row_dir))
    row_back = remote(row_out, row_got, row_out_sems, row_at(row_dir))
    col_back = remote(col_out, col_got, col_out_sems, col_at(col_dir))

    partners = []
    for axis, count, me in (("row", rows, me_row), ("col", cols, me_col)):
        reach = 1
        while reach < count:
            across = me + reach - 2 * reach * ((me // reach) % 2)
            partners.append((across, me_col) if axis == "row" else (me_row, across))
            reach *= 2

    def sum_copy(k, partner=0):
        return pltpu.make_async_remote_copy(
            sum_send.at[k],
            sum_recv.at[k],
            sum_sems.at[0, k],
            sum_sems.at[1, k],
            device_id=partners[partner],
            device_id_type=MESH,
        )

    barrier = pltpu.get_barrier_semaphore()
    row_rounds = rows.bit_length() - 1
    greeted = [row_at(1), row_at(-1), col_at(1)] + ([col_at(-1)] if cols > 2 else [])
    greeted += partners[1:row_rounds] + partners[row_rounds + 1 :]
    for neighbour in greeted:
        pl.semaphore_signal(barrier, inc=1, device_id=neighbour, device_id_type=MESH)
    @pl.loop(0, chunks)
    def _(g):
        for copy in loads(g):
            copy.start()

    iota = functools.partial(lax.broadcasted_iota, jnp.int32)
    to, at = iota((size, size), 0), iota((size, size), 1)
    column = to // tile_rows
    if col_dir > 0:
        kept_columns = tile_cols - width
        column = jnp.where(column < kept_columns, column + width, column - kept_columns)
    split[...] = (at == (to % tile_rows) * tile_cols + column).astype(BF16)
    pl.semaphore_wait(barrier, len(greeted))

    @pl.loop(0, chunks)
    def _(g):
        for copy in loads(g):
            copy.wait()
        for f in range(4):
            own = own_a[g, :, f] if f < 3 else own_b[g]
            tiles = [own[r].astype(F32) for r in range(tile_rows)]
            placed = dot(split[...], jnp.concatenate(tiles, axis=0).astype(BF16), 1, 0)
            placed = placed.astype(BF16)
            tokens[g, f] = placed[:kept]
            col_send[g, f] = placed[kept:]
        col_in(g).start()

    gain_sum[...] = jnp.zeros_like(gain_sum)
    span = table.shape[0]
    shift = (win - 1) * (tile_rows + 1)
    head_count = chunks * heads

    def spot_of(x, y):
        return (span - 1 - y) * tile_rows + span - 1 - x

    flat[...] = jnp.zeros_like(flat)

    @pl.loop(0, span)
    def _(x):
        for y in range(span):
            flat[pl.ds(spot_of(x, y), 1), 0:head_count] = table[x, y : y + 1, :]

    turned = jnp.concatenate([flat[:size].T, flat[size:].T], axis=1)
    across_table[...] = pltpu.roll(turned, 2 * size - shift, 1)

    slots = half * tile_cols

    def is_foreign(r):
        return (r < row_step) if row_dir > 0 else (r >= tile_rows + row_step)

    to, at = iota((slots, size), 0), iota((slots, size), 1)
    column, row = to // half, to % half + first_row
    strip[...] = (at == column * tile_rows + row).astype(BF16)
    row = (row - row_step + tile_rows) % tile_rows
    strip_out[...] = (at == column * tile_rows + row).astype(BF16)

    to, at = iota((size, size + slots), 0), iota((size, size + slots), 1)
    column, row = to // tile_rows, to % tile_rows + row_step
    halo = row - tile_rows if row_dir > 0 else row + half
    outside = (row >= tile_rows) if row_dir > 0 else (row < 0)
    wanted = jnp.where(outside, size + column * half + halo, column * tile_rows + row)
    gather[...] = (at == wanted).astype(BF16)

    skip = tile_cols - width if col_dir > 0 else 0
    to, at = iota((pad, pad + slots), 0), iota((pad, pad + slots), 1)
    column, row = to // tile_rows, to % tile_rows
    wanted = jnp.where(
        is_foreign(row),
        pad + (column + skip) * half + row - first_row,
        column * tile_rows + (row - row_step + tile_rows) % tile_rows,
    )
    scatter_col[...] = (at == wanted).astype(BF16)

    to, at = iota((size, size + slots), 0), iota((size, size + slots), 1)
    row, column = to // tile_cols, to % tile_cols
    if col_dir > 0:
        kept_column, held = column - width, column >= width
        back_column, place_column = column, column - width
    else:
        kept_column, held = column, column < tile_cols - width
        back_column, place_column = column - (tile_cols - width), column + width
    wanted = jnp.where(
        is_foreign(row),
        kept + place_column * half + row - first_row,
        kept_column * tile_rows + (row - row_step + tile_rows) % tile_rows,
    )
    wanted = jnp.where(held, wanted, kept + slots + back_column * tile_rows + row)
    scatter[...] = (at == wanted).astype(BF16)

    row_count, col_count = mask.shape[1], mask.shape[0]
    from_row = lax.rem(row_count + me_row * tile_rows + row_step, row_count)
    from_col = lax.rem(col_count + me_col * tile_cols + jnp.where(steps[1] <= half, steps[1], steps[1] - win), col_count)
    pick = (from_row + iota((row_count, size), 1) % tile_rows) % row_count
    pick = (iota((row_count, size), 0) == pick).astype(F32)
    by_row = dot(mask[...].astype(F32), pick, 1, 0)
    pick = (from_col + iota((col_count, size), 1) // tile_rows) % col_count
    across = jnp.where(iota((col_count, size), 0) == pick, by_row, 0.0)
    across = jnp.sum(across, axis=0, keepdims=True)
    band = (iota((1, size), 1) % tile_rows) // win
    code = jnp.broadcast_to(across * bands + band.astype(F32), (size, size))
    neg[...] = jnp.where(code == code.T, 0.0, NEG_FILL)

    gain_q, gain_k = gains[0:1, :], gains[1:2, :]
    head_lanes = [pl.ds(i * dim, dim) for i in range(heads)]

    def in_place(kept_part, other):
        pair = (kept_part, other)
        return jnp.concatenate(pair[::col_dir], axis=0)

    def merge(g):
        col_in(g).wait_recv()
        for f in range(4):
            both = in_place(tokens[g, f], col_recv[g, f])
            row_send[g, f] = dot(strip[...], both, 1, 0).astype(BF16)
        row_in(g).start()

    def normed(x, gain):
        centred = x - jnp.mean(x, axis=-1, keepdims=True)
        variance = jnp.mean(centred * centred, axis=-1, keepdims=True)
        inv = lax.rsqrt(variance + EPSILON)
        hat = centred * inv
        return hat, inv, (hat * gain).astype(BF16)

    def norm_back(hat, inv, dn, gain):
        g = dn * gain
        first = jnp.mean(g, axis=-1, keepdims=True)
        second = jnp.mean(g * hat, axis=-1, keepdims=True)
        return inv * (g - first - hat * second), jnp.sum(dn * hat, axis=0, keepdims=True)

    sub = 8
    lane_at = lax.broadcasted_iota(jnp.int32, (sub, size), 1)

    def bias_of(head):
        base = jnp.broadcast_to(across_table[pl.ds(head, 1), :], (sub, 2 * size))
        base = pltpu.roll(base, 0, 1, stride=1, stride_axis=0)
        low, high = base[:, :size], base[:, size:]
        blocks = [low]
        for b in range(1, size // sub):
            blocks.append(
                jnp.where(
                    lane_at < b * sub,
                    pltpu.roll(high, b * sub, 1),
                    pltpu.roll(low, b * sub, 1),
                )
            )
        return jnp.concatenate(blocks, axis=0)

    def fold(head, ds):
        low, high = ds[:sub], jnp.zeros((sub, size), F32)
        for b in range(1, size // sub):
            moved = pltpu.roll(ds[b * sub : (b + 1) * sub], size - b * sub, 1)
            inside = lane_at < size - b * sub
            low = low + jnp.where(inside, moved, 0.0)
            high = high + jnp.where(inside, 0.0, moved)
        skew[0, pl.ds(head * sub, sub), :] = low
        skew[1, pl.ds(head * sub, sub), :] = high

    def softmax(s):
        e = jnp.exp(s - jnp.max(s, axis=-1, keepdims=True))
        return e * (1.0 / jnp.sum(e, axis=-1, keepdims=True))

    def attend(g, fields):
        each = range(heads)
        split_heads = [[x[:, i * dim : (i + 1) * dim] for x in fields] for i in each]
        q, k, v, ct = zip(*split_heads)
        bias = [bias_of(g * heads + i) + neg[...] for i in each]
        qs = [normed(x.astype(F32), gain_q) for x in q]
        ks = [normed(x.astype(F32), gain_k) for x in k]
        qn, kn = [x[2] for x in qs], [x[2] for x in ks]
        s = [dot(qn[i], kn[i], 1, 1) for i in each]
        dp = [dot(ct[i], v[i], 1, 1) for i in each]
        p = [softmax(s[i] * scale + bias[i]) for i in each]
        ds = [p[i] * (dp[i] - jnp.sum(p[i] * dp[i], axis=-1, keepdims=True)) for i in each]
        pb = [x.astype(BF16) for x in p]
        dsb = [x.astype(BF16) for x in ds]
        dqn = [dot(dsb[i], kn[i], 1, 0) * scale for i in each]
        dkn = [dot(dsb[i], qn[i], 0, 0) * scale for i in each]
        att = [dot(pb[i], v[i], 1, 0) for i in each]
        dv = [dot(pb[i], ct[i], 0, 0) for i in each]
        total = 0.0
        for i, at in enumerate(head_lanes):
            fold(g * heads + i, ds[i])
            dq, gq = norm_back(qs[i][0], qs[i][1], dqn[i], gain_q)
            dk, gk = norm_back(ks[i][0], ks[i][1], dkn[i], gain_k)
            for f, value in enumerate((att[i], dq, dk, dv[i])):
                results[g, f, :, at] = value.astype(BF16)
            total = total + jnp.concatenate([gq, gk], axis=0)
        gain_sum[...] += total

    def compute(g):
        row_in(g).wait_recv()
        fields = []
        for f in range(4):
            both = in_place(tokens[g, f], col_recv[g, f])
            both = jnp.concatenate([both, row_recv[g, f]], axis=0)
            fields.append(dot(gather[...], both, 1, 0).astype(BF16))
        attend(g, fields)
        for f in range(4):
            row_out[g, f] = dot(strip_out[...], results[g, f], 1, 0).astype(BF16)
        row_back(g).start()

    ours, theirs = pl.ds(0, kept), pl.ds(kept, pad)
    if col_dir < 0:
        ours, theirs = pl.ds(pad, kept), pl.ds(0, pad)

    def give_back(g):
        row_back(g).wait_recv()
        for f in range(4):
            both = jnp.concatenate([results[g, f, theirs], row_got[g, f]], axis=0)
            col_out[g, f] = dot(scatter_col[...], both, 1, 0).astype(BF16)
        col_back(g).start()

    def final(g):
        col_back(g).wait_recv()
        for f in range(4):
            parts = [results[g, f, ours], row_got[g, f], col_got[g, f]]
            value = dot(scatter[...], jnp.concatenate(parts, axis=0), 1, 0)
            for r in range(tile_rows):
                tile = value[r * tile_cols : (r + 1) * tile_cols].astype(BF16)
                if f == 0:
                    att_out[r, :, lane(g)] = tile
                else:
                    dqkv_out[r, f - 1, :, lane(g)] = tile

    def first_sum():
        total = jnp.zeros((head_count, 2 * size), F32)
        for j in range(sub):
            part = [skew[i, pl.ds(j, head_count, stride=sub), :] for i in range(2)]
            part = jnp.concatenate(part, axis=1)
            total = total + (pltpu.roll(part, 2 * size - j, 1) if j else part)
        total = pltpu.roll(total, shift, 1)
        gain = jnp.concatenate([gain_sum[0:1, :], gain_sum[1:2, :]], axis=1)
        rest = jnp.zeros((sum_send.shape[1] - head_count - 1, 2 * size), F32)
        sum_send[0] = jnp.concatenate([total, gain, rest], axis=0)
        sum_copy(0, 0).start()

    def next_sum(k):
        sum_copy(k - 1).wait_recv()
        total = sum_send[k - 1] + sum_recv[k - 1]
        if k < len(partners):
            sum_send[k] = total
            sum_copy(k, k).start()
            return
        dgain[0:1, :] = total[head_count : head_count + 1, :dim]
        dgain[1:2, :] = total[head_count : head_count + 1, dim:]
        square = jnp.concatenate(
            [total, jnp.zeros((size - total.shape[0], 2 * size), F32)], axis=0
        )
        flat[0:size, :] = square[:, :size].T
        flat[size : 2 * size, :] = square[:, size:].T

        @pl.loop(0, span)
        def _(x):
            for y in range(span):
                dtable[x, y : y + 1, :] = flat[pl.ds(spot_of(x, y), 1), 0:head_count]

    lag_a = min(LAG_COMPUTE, chunks)
    lag_b = lag_a + LAG_RETURN
    lag_c = lag_b + LAG_FINAL

    rounds = len(partners)
    done = chunks + lag_a

    @pl.loop(0, max(chunks + lag_c, done + rounds + 1))
    def _(t):
        @pl.when(t < chunks)
        def _():
            merge(t)

        @pl.when(jnp.logical_and(t >= lag_b, t < chunks + lag_b))
        def _():
            give_back(t - lag_b)

        @pl.when(jnp.logical_and(t >= lag_a, t < chunks + lag_a))
        def _():
            compute(t - lag_a)

        @pl.when(jnp.logical_and(t >= lag_c, t < chunks + lag_c))
        def _():
            final(t - lag_c)

        for k in range(rounds + 1):

            @pl.when(t == done - 1 + k)
            def _(k=k):
                if k == 0:
                    first_sum()
                else:
                    next_sum(k)

    @pl.loop(0, chunks)
    def _(g):
        for copy in (col_in, row_in, row_back, col_back):
            copy(g).wait_send()

    @pl.loop(0, rounds)
    def _(k):
        sum_copy(k).wait_send()


def window_pass(
    steps, qkv, cot, gains, table, mask, *, row_dir, col_dir, width, win, dim, call_id
):
    tile_rows, fields, tile_cols, features = qkv.shape
    head_count = features // dim
    heads = HEADS if head_count % HEADS == 0 else 1
    lanes = heads * dim
    chunks = head_count // heads
    half = win // 2
    slots = half * tile_cols
    size = tile_rows * tile_cols
    pad = width * tile_rows
    rounds = sum(lax.axis_size(a).bit_length() - 1 for a in ("row", "col"))
    sum_rows = -(-(head_count + 1) // 8) * 8
    any_spec = pl.BlockSpec(memory_space=pl.ANY)
    vmem_spec = pl.BlockSpec(memory_space=pltpu.VMEM)
    vmem = pltpu.VMEM
    dma = pltpu.SemaphoreType.DMA
    return pl.pallas_call(
        functools.partial(
            window_kernel,
            row_dir=row_dir,
            col_dir=col_dir,
            width=width,
            win=win,
            heads=heads,
            dim=dim,
        ),
        in_specs=[pl.BlockSpec(memory_space=pltpu.SMEM), any_spec, any_spec]
        + [vmem_spec] * 3,
        out_specs=[vmem_spec] * 4,
        out_shape=[
            jax.ShapeDtypeStruct(cot.shape, BF16),
            jax.ShapeDtypeStruct(qkv.shape, BF16),
            jax.ShapeDtypeStruct((2, dim), F32),
            jax.ShapeDtypeStruct(table.shape, F32),
        ],
        scratch_shapes=[
            vmem((chunks, tile_rows, fields, tile_cols, lanes), BF16),
            vmem((chunks, tile_rows, tile_cols, lanes), BF16),
            vmem((chunks, 4, size - pad, lanes), BF16),
            vmem((chunks, 4, pad, lanes), BF16),
            vmem((chunks, 4, pad, lanes), BF16),
            vmem((chunks, 4, slots, lanes), BF16),
            vmem((chunks, 4, slots, lanes), BF16),
            vmem((chunks, 4, size, lanes), BF16),
            vmem((chunks, 4, slots, lanes), BF16),
            vmem((chunks, 4, slots, lanes), BF16),
            vmem((chunks, 4, pad, lanes), BF16),
            vmem((chunks, 4, pad, lanes), BF16),
            vmem((size, size), F32),
            vmem((size, size), BF16),
            vmem((slots, size), BF16),
            vmem((size, size + slots), BF16),
            vmem((slots, size), BF16),
            vmem((pad, pad + slots), BF16),
            vmem((size, size + slots), BF16),
            vmem((2, dim), F32),
            vmem((2 * size, size), F32),
            vmem((size, 2 * size), F32),
            vmem((2, head_count * 8, size), F32),
            vmem((rounds, sum_rows, 2 * size), F32),
            vmem((rounds, sum_rows, 2 * size), F32),
            dma((2, chunks)),
            dma((2, chunks)),
            dma((2, chunks)),
            dma((2, chunks)),
            dma((2, chunks)),
            dma((2, rounds)),
        ],
        compiler_params=pltpu.CompilerParams(
            collective_id=call_id, has_side_effects=True, vmem_limit_bytes=60 * 1024 * 1024
        ),
        name="windows",
    )(steps, qkv, cot, gains, table, mask)


def local(qkv, cotangent, norm_gains, rel_table, shifts, mask_ids):
    head_count, span, _ = rel_table.shape
    dim = qkv.shape[3] // head_count
    win = (span + 1) // 2
    half = win // 2
    branches = []
    for row_dir in (1, -1):
        for col_step in (*range(1, half + 1), *range(1 - half, 0)):
            branches.append(
                functools.partial(
                    window_pass,
                    row_dir=row_dir,
                    col_dir=1 if col_step > 0 else -1,
                    width=abs(col_step),
                    win=win,
                    dim=dim,
                    call_id=len(branches),
                )
            )
    index = jnp.where(shifts[0] <= half, 0, win - 1) + shifts[1] - 1
    att, dqkv, dgain, dtable = lax.switch(
        index,
        branches,
        shifts,
        qkv.transpose(0, 2, 1, 3),
        cotangent,
        norm_gains,
        rel_table.transpose(1, 2, 0),
        mask_ids.T,
    )
    return (att, dqkv.transpose(0, 2, 1, 3), dgain, dtable.transpose(2, 0, 1))


def solution(mesh):
    placed = (P("row", "col", None, None), P("row", "col", None), P(), P(), P(), P())
    return jax.shard_map(
        local,
        mesh=mesh,
        in_specs=placed,
        out_specs=(P("row", "col", None), P("row", "col", None, None), P(), P()),
        check_vma=False,
    )
```
